32 devices in a mesh: wide: 8 (over y, x, core), narrow: 4 (over z).
Axes of the slice: x: 2, y: 2, z: 4, core: 2. Of those that a mesh axis runs over, the one named last changes fastest.
Arguments:
- first_state: float32 [2, 32768, 1024], P(None, ('wide', 'narrow')), may hold values from -100 to 100
- second_state: float32 [2, 32768, 1024], P(None, ('wide', 'narrow')), may hold values from -200 to 200
- place_first: int32 [32768], replicated, may hold values from 0 to 32767, as said below
- place_second: int32 [32768], replicated, may hold values from 0 to 32767, as said below
Outputs:
- aligned: float32 [2, 32768, 1024], P(None, ('wide', 'narrow'))
- intersection: float32 [2], replicated
- norms: float32 [2], replicated
The draws below stay inside these ranges and needn't reach their ends.
Inputs may be any that keep to these rules, and one draw needn't show every extreme that they name: Each of place_first and place_second maps a logical block index to a storage block index by a permutation of the index's bits. Every logical bit that selects a device (the high bits of a storage index above its position within a device) in one state's order selects a block within a device in the other's, so each device holds exactly 32 blocks of the second state that the first state's order places on any given device. `place_second`: drawn together with place_first under the rule stated there.
All inputs are finite; a program needn't handle non-finite values.
Results may differ from the reference program's by a relative error of at most 0.00002.
Values sent between devices are 32-bit elements; how exact they have to be, the bound alone decides.
A program may use at most 128 MiB of HBM per device.

```python
import math
import jax
import jax.numpy as jnp
from jax import lax

BLOCK = 1024
BLOCKS_DEV = 1024
BLOCKS = 32768
AMPS = 33554432


def block_maps(key):
    block_bits = int(BLOCKS).bit_length() - 1
    global_bits = int(BLOCKS // BLOCKS_DEV).bit_length() - 1
    local_bits = block_bits - global_bits
    sigma = jax.random.permutation(jax.random.fold_in(key, 11), block_bits).astype(jnp.int32)
    device_first = sigma[:global_bits]
    device_second = sigma[global_bits:2 * global_bits]
    others = sigma[2 * global_bits:]
    order_first = jax.random.permutation(jax.random.fold_in(key, 12), local_bits).astype(jnp.int32)
    order_second = jax.random.permutation(jax.random.fold_in(key, 13), local_bits).astype(jnp.int32)
    local_first = jnp.concatenate([device_second, others])[order_first]
    local_second = jnp.concatenate([device_first, others])[order_second]
    map_first = jnp.concatenate([local_first, device_first]).astype(jnp.int32)
    map_second = jnp.concatenate([local_second, device_second]).astype(jnp.int32)
    return (map_first, map_second)


def storage_of(logical, bit_map):
    block_bits = int(BLOCKS).bit_length() - 1
    store = jnp.zeros_like(logical)
    for level in range(block_bits):
        store = store + jnp.left_shift(jnp.right_shift(logical, bit_map[level]) & 1, level)
    return store.astype(jnp.int32)


def logical_of(store, bit_map):
    block_bits = int(BLOCKS).bit_length() - 1
    logical = jnp.zeros_like(store)
    for level in range(block_bits):
        logical = logical + jnp.left_shift(jnp.right_shift(store, level) & 1, bit_map[level])
    return logical.astype(jnp.int32)


def block_scale(key, expo):
    steps = jnp.arange(BLOCKS, dtype=jnp.float32) / float(max(BLOCKS - 1, 1))
    rising = jnp.exp(expo * math.log(3.0) * steps)
    spread = jnp.exp(jax.random.uniform(key, (BLOCKS,), jnp.float32, 0.0, 0.5 * math.log(10.0)))
    return rising * spread


def base_normals(key):
    return jnp.clip(jax.random.normal(jax.random.fold_in(key, 31), (2, BLOCKS, BLOCK), jnp.float32), -6.0, 6.0)


def draw_place_first(key, part):
    map_first, map_second = block_maps(key)
    return storage_of(jnp.arange(BLOCKS, dtype=jnp.int32), map_first)


def draw_place_second(key, part):
    map_first, map_second = block_maps(key)
    return storage_of(jnp.arange(BLOCKS, dtype=jnp.int32), map_second)


def draw_first_state(key, part):
    expo = 0.5
    scale_first = block_scale(jax.random.fold_in(key, 21), expo)
    return base_normals(key) * scale_first[None, :, None]


def draw_second_state(key, part):
    expo = 0.5
    map_first, map_second = block_maps(key)
    logical = logical_of(jnp.arange(BLOCKS, dtype=jnp.int32), map_second)
    rows_first = storage_of(logical, map_first)
    shared = jnp.take(base_normals(key), rows_first, axis=1)
    angles = jax.random.uniform(jax.random.fold_in(key, 41), (BLOCKS,), jnp.float32, 0.3, 1.2)
    cosine = jnp.cos(angles)[:, None]
    sine = jnp.sin(angles)[:, None]
    turned = jnp.stack([cosine * shared[0] - sine * shared[1], sine * shared[0] + cosine * shared[1]])
    noise = jnp.clip(jax.random.normal(jax.random.fold_in(key, 32), (2, BLOCKS, BLOCK), jnp.float32), -6.0, 6.0)
    scale_second = block_scale(jax.random.fold_in(key, 22), expo)
    return (0.6 * turned + 0.8 * noise) * scale_second[None, :, None]


def setup_inputs(seed: int = 0) -> dict:
    key_of = jax.random.split(jax.random.key(seed), 5)
    first_state = draw_first_state(jax.random.fold_in(key_of[4], 71), 0)
    second_state = draw_second_state(jax.random.fold_in(key_of[4], 71), 0)
    place_first = draw_place_first(jax.random.fold_in(key_of[4], 71), 0)
    place_second = draw_place_second(jax.random.fold_in(key_of[4], 71), 0)
    return dict(first_state=first_state, second_state=second_state, place_first=place_first, place_second=place_second)


def reference(first_state, second_state, place_first, place_second):
    index_list = jnp.arange(BLOCKS, dtype=jnp.int32)
    logical_first = jnp.zeros((BLOCKS,), jnp.int32).at[place_first].set(index_list)
    source_blocks = place_second[logical_first].astype(jnp.int32)
    gathered = jnp.take(second_state, source_blocks, axis=1)
    amp_total = float(AMPS)
    first_sq = jnp.sum(lax.optimization_barrier(jnp.sum(first_state * first_state, axis=2)))
    second_sq = jnp.sum(lax.optimization_barrier(jnp.sum(second_state * second_state, axis=2)))
    real_sum = jnp.sum(lax.optimization_barrier(jnp.sum(first_state[0] * gathered[0] + first_state[1] * gathered[1], axis=1)))
    imag_sum = jnp.sum(lax.optimization_barrier(jnp.sum(first_state[0] * gathered[1] - first_state[1] * gathered[0], axis=1)))
    mean_first = first_sq / amp_total
    mean_second = second_sq / amp_total
    aligned = gathered / jnp.sqrt(mean_second + 1e-06)
    intersection = jnp.stack([real_sum, imag_sum]) / amp_total / jnp.sqrt((mean_first + 1e-06) * (mean_second + 1e-06))
    norms = jnp.stack([mean_first, mean_second])
    return (aligned, intersection, norms)
```

```python
import functools

import jax
import jax.numpy as jnp
from jax import lax
from jax.experimental import pallas as pl
from jax.experimental.pallas import tpu as pltpu
from jax.sharding import PartitionSpec as P

MESH = pl.DeviceIdType.MESH
SUB = 8
LANE = 128


def row_weight(one_hot):
    return jnp.where(one_hot < SUB, one_hot, one_hot * SUB)


def bits(count):
    return count.bit_length() - 1


def table(ref, base, weights, start=0):
    ref[base] = jnp.int32(start)
    for level, weight in enumerate(weights):
        for low in range(1 << level):
            ref[base + (1 << level) + low] = ref[base + low] + weight


def build_tables(place_f, place_s, blocks_dev, devices, me, share, rows_out, rows_in, back):
    levels = bits(blocks_dev * devices)
    zero = jnp.int32(0)
    dev_out = [zero] * bits(devices)
    dev_in = [zero] * bits(devices)
    k_out = [zero] * bits(share)
    k_in = [zero] * bits(share)
    slot_back = [zero] * bits(blocks_dev)
    unit = jnp.int32(1)
    for level in range(levels):
        f = place_f(level)
        s = place_s(level)
        f_dev = f >> bits(blocks_dev)
        s_dev = s >> bits(blocks_dev)
        both = (f_dev == 0) & (s_dev == 0)
        for j in range(bits(devices)):
            dev_out[j] = dev_out[j] + jnp.where(f_dev == (1 << j), row_weight(s), 0)
            dev_in[j] = dev_in[j] + jnp.where(s_dev == (1 << j), row_weight(f), 0)
        for i in range(bits(share)):
            here = both & (unit == (1 << i))
            k_out[i] = k_out[i] + jnp.where(here, row_weight(s), 0)
            k_in[i] = k_in[i] + jnp.where(here, row_weight(f), 0)
        toward = jnp.where((s_dev & me) == 0, s_dev, -s_dev)
        packed = jnp.where(both, unit * SUB, toward * (2 * share * SUB))
        for p in range(bits(blocks_dev)):
            slot_back[p] = slot_back[p] + jnp.where(f == (1 << p), packed, 0)
        unit = jnp.where(both, unit * 2, unit)
    table(rows_out, 0, dev_out)
    table(rows_out, devices, k_out)
    table(rows_in, 0, dev_in)
    table(rows_in, devices, k_in)
    table(back, 0, slot_back[:bits(SUB)], me * (2 * share * SUB))
    table(back, SUB, slot_back[bits(SUB):])


def exchange(sizes, blocks_dev, share, amp_total, place_first, place_second, first_hbm, second_hbm,
             held, means,
             first, outgoing, arrived, stats, totals, powers, rows_out, rows_in, back,
             load_sem, place_sem, send_sem, recv_sem, sum_send, sum_recv):
    wide_count, narrow_count = sizes
    devices = wide_count * narrow_count
    levels = bits(blocks_dev * devices)
    me_w = lax.axis_index("wide")
    me_n = lax.axis_index("narrow")
    me = me_w * narrow_count + me_n
    part_rows = blocks_dev * SUB
    message = 2 * share * SUB

    lines = [0] + [1 << line for line in range(levels - bits(LANE))]
    fetches = []
    for which, place in enumerate((place_first, place_second)):
        for at, line in enumerate(lines):
            fetches.append(pltpu.make_async_copy(
                place.at[pl.ds(line, 1), :], powers.at[which, pl.ds(at, 1), :],
                place_sem.at[which * len(lines) + at]))
    load_second = pltpu.make_async_copy(second_hbm, held, load_sem.at[0])
    load_first = pltpu.make_async_copy(first_hbm, first, load_sem.at[1])
    for fetch in fetches:
        fetch.start()
    load_second.start()

    def partner(offset):
        return (jnp.bitwise_xor(me_w, offset // narrow_count),
                jnp.bitwise_xor(me_n, lax.rem(offset, narrow_count)))

    def other(offset):
        other_w, other_n = partner(offset)
        return other_w * narrow_count + other_n

    barrier = pltpu.get_barrier_semaphore()

    @pl.loop(1, devices)
    def _(offset):
        pl.semaphore_signal(barrier, inc=1, device_id=partner(offset), device_id_type=MESH)

    for fetch in fetches:
        fetch.wait()

    def place_of(which):
        def entry(level):
            if (1 << level) < LANE:
                return powers[which, 0, 1 << level]
            return powers[which, 1 + level - bits(LANE), 0]
        return entry

    build_tables(place_of(0), place_of(1), blocks_dev, devices, me, share, rows_out, rows_in, back)
    load_second.wait()
    load_first.start()
    pl.semaphore_wait(barrier, devices - 1)

    last = narrow_count - 1
    inner = (me_n != 0) & (me_n != last)
    flip = jnp.where(lax.rem(me_w, 2) == 1, wide_count - 1, 0)

    def offset_of(seq):
        group = seq // narrow_count
        turn = lax.rem(seq, narrow_count)
        far = jnp.where(inner, jnp.where(turn == 0, last, turn), turn + 1)
        away = jnp.bitwise_xor(group, flip) * narrow_count + far
        return jnp.where(turn < last, away, (group + 1) * narrow_count)

    def rows_at(ref, offset):
        return ref.at[pl.ds(pl.multiple_of(offset * message, message), message), :]

    def block_at(offset, part, k):
        return pl.ds(pl.multiple_of(offset * message + (part * share + k) * SUB, SUB), SUB)

    def block_copy(offset):
        return pltpu.make_async_remote_copy(
            src_ref=rows_at(outgoing, offset), dst_ref=rows_at(arrived, offset),
            send_sem=send_sem.at[offset], recv_sem=recv_sem.at[offset],
            device_id=partner(offset), device_id_type=MESH)

    def pack(offset, out):
        base = rows_out[other(offset)]

        def row(k, carry):
            start = base + rows_out[devices + k]
            for part in range(2):
                out[block_at(offset, part, k), :] = held[pl.ds(start + part * part_rows, SUB, stride=SUB), :]
            return carry

        lax.fori_loop(0, share, row, 0, unroll=min(8, share))

    def pack_and_send(seq):
        pack(offset_of(seq), outgoing)
        block_copy(offset_of(seq - 1)).start()

    def sum_copy(kind, offset):
        return pltpu.make_async_remote_copy(
            src_ref=stats.at[kind], dst_ref=totals.at[kind, me],
            send_sem=sum_send.at[kind, offset], recv_sem=sum_recv.at[kind, offset],
            device_id=partner(offset), device_id_type=MESH)

    def keep_sums(kind, sums):
        for which in range(2):
            stats[kind, pl.ds(which, 1), :] = jnp.sum(sums[which], axis=0, keepdims=True)
        totals[kind, me] = stats[kind]

    def send_sums(kind):
        @pl.loop(1, devices)
        def _(offset):
            sum_copy(kind, offset).start()

    def summed(kind):
        @pl.loop(1, devices)
        def _(offset):
            sum_copy(kind, offset).wait()

        total = jnp.sum(totals[kind], axis=0)
        return [jnp.broadcast_to(jnp.sum(total[which:which + 1]) / amp_total, (SUB, LANE)) for which in range(2)]

    early = devices // 2
    pack(offset_of(0), outgoing)
    pl.loop(1, early)(pack_and_send)

    load_first.wait()
    chunk = 16 * SUB

    def squares(i, carry):
        at = pl.multiple_of(i * chunk, chunk)
        a = first[pl.ds(at, chunk), :].reshape(chunk // SUB, SUB, LANE)
        b = held[pl.ds(at, chunk), :].reshape(chunk // SUB, SUB, LANE)
        return carry[0] + jnp.sum(a * a, axis=0), carry[1] + jnp.sum(b * b, axis=0)

    zero = jnp.zeros((SUB, LANE), jnp.float32)
    keep_sums(0, lax.fori_loop(0, 2 * part_rows // chunk, squares, (zero, zero)))
    pack_and_send(early)
    send_sums(0)
    pl.loop(early + 1, devices - 1)(pack_and_send)
    pack(0, arrived)
    block_copy(offset_of(devices - 2)).start()

    def dots(offset, carry):
        base = rows_in[other(offset)]

        def row(k, carry):
            real, imag = carry
            start = base + rows_in[devices + k]
            f_re = first[pl.ds(start, SUB, stride=SUB), :]
            f_im = first[pl.ds(start + part_rows, SUB, stride=SUB), :]
            g_re = arrived[block_at(offset, 0, k), :]
            g_im = arrived[block_at(offset, 1, k), :]
            return real + (f_re * g_re + f_im * g_im), imag + (f_re * g_im - f_im * g_re)

        return lax.fori_loop(0, share, row, carry, unroll=min(8, share))

    def take(seq, carry):
        offset = offset_of(seq)
        block_copy(offset).wait_recv()
        return dots(offset, carry)

    keep_sums(1, lax.fori_loop(0, devices - 1, take, dots(0, (zero, zero))))

    @pl.loop(1, devices)
    def _(offset):
        block_copy(offset).wait_send()

    send_sums(1)
    mean_first, mean_second = summed(0)
    scale = 1.0 / jnp.sqrt(mean_second + 1e-06)

    def group(i, carry):
        base = pl.multiple_of(i * (SUB * SUB), SUB * SUB)
        high = back[SUB + i]
        for r in range(SUB):
            start = high + back[r]
            for part in range(2):
                block = arrived[pl.ds(start + part * (share * SUB), SUB), :]
                held[pl.ds(base + part * part_rows + r, SUB, stride=SUB), :] = block * scale
        return carry

    lax.fori_loop(0, blocks_dev // SUB, group, 0, unroll=2)

    both = jnp.sqrt((mean_first + 1e-06) * (mean_second + 1e-06))
    real, imag = summed(1)
    for row, value in enumerate((real / both, imag / both, mean_first, mean_second)):
        means[pl.ds(row, 1), :] = value[:1]


def store(pieces, held, means, out_hbm, intersection, norms, out_sem):
    piece = held.shape[0] // pieces
    copies = [pltpu.make_async_copy(held.at[pl.ds(at * piece, piece), :], out_hbm.at[pl.ds(at * piece, piece), :],
                                    out_sem.at[at]) for at in range(pieces)]
    for copy in copies:
        copy.start()
    for which in range(2):
        intersection[which] = means[which, 0]
        norms[which] = means[2 + which, 0]
    for copy in copies:
        copy.wait()


def local(first_state, second_state, place_first, place_second):
    blocks_dev = first_state.shape[1]
    block = first_state.shape[2]
    wide_count = lax.axis_size("wide")
    narrow_count = lax.axis_size("narrow")
    devices = wide_count * narrow_count
    share = blocks_dev // devices
    lines = 1 + bits(blocks_dev * devices) - bits(LANE)

    def tiles(state):
        split = state.reshape(2, blocks_dev // SUB, SUB, block // LANE, LANE)
        return split.transpose(0, 1, 3, 2, 4).reshape(2 * blocks_dev * SUB, LANE)

    pieces = 8
    rows = (2 * blocks_dev * SUB, LANE)
    any_spec = pl.BlockSpec(memory_space=pl.ANY)
    hbm_spec = pl.BlockSpec(memory_space=pltpu.HBM)
    vmem_spec = pl.BlockSpec(memory_space=pltpu.VMEM)
    smem_spec = pl.BlockSpec(memory_space=pltpu.SMEM)
    held, means = pl.pallas_call(
        functools.partial(exchange, (wide_count, narrow_count), blocks_dev, share,
                          float(blocks_dev * devices * block)),
        out_shape=(pltpu.VMEM(rows, jnp.float32), pltpu.VMEM((SUB, LANE), jnp.float32)),
        in_specs=[hbm_spec] * 4,
        out_specs=(vmem_spec, vmem_spec),
        scratch_shapes=[pltpu.VMEM(rows, jnp.float32)] * 3 + [
            pltpu.VMEM((2, 2, LANE), jnp.float32),
            pltpu.VMEM((2, devices, 2, LANE), jnp.float32),
            pltpu.SMEM((2, lines, LANE), jnp.int32),
            pltpu.SMEM((devices + share,), jnp.int32),
            pltpu.SMEM((devices + share,), jnp.int32),
            pltpu.SMEM((SUB + blocks_dev // SUB,), jnp.int32),
            pltpu.SemaphoreType.DMA((2,)),
            pltpu.SemaphoreType.DMA((2 * lines,)),
            pltpu.SemaphoreType.DMA((devices,)),
            pltpu.SemaphoreType.DMA((devices,)),
            pltpu.SemaphoreType.DMA((2, devices)),
            pltpu.SemaphoreType.DMA((2, devices)),
        ],
        compiler_params=pltpu.CompilerParams(
            collective_id=0, has_side_effects=True, vmem_limit_bytes=28 << 20),
        name="exchange",
    )(*(pltpu.with_memory_space_constraint(operand, pltpu.HBM) for operand in (
        place_first.reshape(-1, LANE), place_second.reshape(-1, LANE), tiles(first_state), tiles(second_state))))
    aligned, intersection, norms = pl.pallas_call(
        functools.partial(store, pieces),
        out_shape=(jax.ShapeDtypeStruct(rows, jnp.float32),
                   jax.ShapeDtypeStruct((2,), jnp.float32),
                   jax.ShapeDtypeStruct((2,), jnp.float32)),
        in_specs=[vmem_spec] * 2,
        out_specs=(any_spec, smem_spec, smem_spec),
        scratch_shapes=[pltpu.SemaphoreType.DMA((pieces,))],
        compiler_params=pltpu.CompilerParams(vmem_limit_bytes=1 << 20),
        name="store",
    )(held, means)
    aligned = aligned.reshape(2, blocks_dev // SUB, block // LANE, SUB, LANE)
    aligned = aligned.transpose(0, 1, 3, 2, 4).reshape(2, blocks_dev, block)
    return (aligned, intersection, norms)


def solution(mesh):
    return jax.shard_map(
        local,
        mesh=mesh,
        in_specs=(P(None, ("wide", "narrow"), None), P(None, ("wide", "narrow"), None), P(), P()),
        out_specs=(P(None, ("wide", "narrow"), None), P(), P()),
        check_vma=False,
    )
```

```python
import functools

import jax
import jax.numpy as jnp
from jax import lax
from jax.experimental import pallas as pl
from jax.experimental.pallas import tpu as pltpu
from jax.sharding import PartitionSpec as P

MESH = pl.DeviceIdType.MESH
SUB = 8
LANE = 128


def row_weight(one_hot):
    return jnp.where(one_hot < SUB, one_hot, one_hot * SUB)


def bits(count):
    return count.bit_length() - 1


def table(ref, base, weights, start=0):
    ref[base] = jnp.int32(start)
    for level, weight in enumerate(weights):
        for low in range(1 << level):
            ref[base + (1 << level) + low] = ref[base + low] + weight


def build_tables(place_f, place_s, blocks_dev, devices, me, share, rows_out, rows_in, back):
    levels = bits(blocks_dev * devices)
    zero = jnp.int32(0)
    dev_out = [zero] * bits(devices)
    dev_in = [zero] * bits(devices)
    k_out = [zero] * bits(share)
    k_in = [zero] * bits(share)
    slot_back = [zero] * bits(blocks_dev)
    unit = jnp.int32(1)
    for level in range(levels):
        f = place_f(level)
        s = place_s(level)
        f_dev = f >> bits(blocks_dev)
        s_dev = s >> bits(blocks_dev)
        both = (f_dev == 0) & (s_dev == 0)
        for j in range(bits(devices)):
            dev_out[j] = dev_out[j] + jnp.where(f_dev == (1 << j), row_weight(s), 0)
            dev_in[j] = dev_in[j] + jnp.where(s_dev == (1 << j), row_weight(f), 0)
        for i in range(bits(share)):
            here = both & (unit == (1 << i))
            k_out[i] = k_out[i] + jnp.where(here, row_weight(s), 0)
            k_in[i] = k_in[i] + jnp.where(here, row_weight(f), 0)
        toward = jnp.where((s_dev & me) == 0, s_dev, -s_dev)
        packed = jnp.where(both, unit * SUB, toward * (2 * share * SUB))
        for p in range(bits(blocks_dev)):
            slot_back[p] = slot_back[p] + jnp.where(f == (1 << p), packed, 0)
        unit = jnp.where(both, unit * 2, unit)
    table(rows_out, 0, dev_out)
    table(rows_out, devices, k_out)
    table(rows_in, 0, dev_in)
    table(rows_in, devices, k_in)
    table(back, 0, slot_back[:bits(SUB)], me * (2 * share * SUB))
    table(back, SUB, slot_back[bits(SUB):])


def exchange(sizes, blocks_dev, share, amp_total, place_first, place_second, first_hbm, second_hbm,
             held_re, held_im, sums,
             first, outgoing, arrived, stats, totals, powers, rows_out, rows_in, back,
             load_sem, place_sem, send_sem, recv_sem, sum_send, sum_recv):
    wide_count, narrow_count = sizes
    devices = wide_count * narrow_count
    levels = bits(blocks_dev * devices)
    me_w = lax.axis_index("wide")
    me_n = lax.axis_index("narrow")
    me = me_w * narrow_count + me_n
    part_rows = blocks_dev * SUB
    half = share * SUB
    message = 2 * half
    held = (held_re, held_im)

    def partner(offset):
        return (jnp.bitwise_xor(me_w, offset // narrow_count),
                jnp.bitwise_xor(me_n, lax.rem(offset, narrow_count)))

    def other(offset):
        other_w, other_n = partner(offset)
        return other_w * narrow_count + other_n

    load_second = [pltpu.make_async_copy(second_hbm.at[pl.ds(part * part_rows, part_rows), :], held[part],
                                         load_sem.at[part]) for part in range(2)]
    load_first = pltpu.make_async_copy(first_hbm, first, load_sem.at[2])
    load_second[0].start()
    barrier = pltpu.get_barrier_semaphore()

    @pl.loop(1, devices)
    def _(offset):
        pl.semaphore_signal(barrier, inc=1, device_id=partner(devices - offset), device_id_type=MESH)

    lines = [0] + [1 << line for line in range(levels - bits(LANE))]
    for which, place in enumerate((place_first, place_second)):
        for at, line in enumerate(lines):
            pltpu.make_async_copy(place.at[pl.ds(line, 1), :], powers.at[which, pl.ds(at, 1), :],
                                  place_sem.at[which]).start()
    load_second[1].start()
    for which, place in enumerate((place_first, place_second)):
        pltpu.make_async_copy(place.at[pl.ds(0, len(lines)), :], powers.at[which], place_sem.at[which]).wait()

    def place_of(which):
        def entry(level):
            if (1 << level) < LANE:
                return powers[which, 0, 1 << level]
            return powers[which, 1 + level - bits(LANE), 0]
        return entry

    build_tables(place_of(0), place_of(1), blocks_dev, devices, me, share, rows_out, rows_in, back)

    last = narrow_count - 1
    inner = (me_n != 0) & (me_n != last)
    flip = jnp.where(lax.rem(me_w, 2) == 1, wide_count - 1, 0)

    def offset_of(seq):
        group = seq // narrow_count
        turn = lax.rem(seq, narrow_count)
        far = jnp.where(inner, jnp.where(turn == 0, last, turn), turn + 1)
        away = jnp.bitwise_xor(group, flip) * narrow_count + far
        return jnp.where(turn < last, away, (group + 1) * narrow_count)

    def rows_at(ref, offset):
        return ref.at[pl.ds(pl.multiple_of(offset * message, message), message), :]

    def block_at(offset, part, k):
        return pl.ds(pl.multiple_of(offset * message + (part * share + k) * SUB, SUB), SUB)

    def half_copy(offset, part):
        at = pl.ds(pl.multiple_of(offset * message + part * half, half), half)
        return pltpu.make_async_remote_copy(
            src_ref=outgoing.at[at, :], dst_ref=arrived.at[at, :],
            send_sem=send_sem.at[0], recv_sem=recv_sem.at[offset],
            device_id=partner(offset), device_id_type=MESH)

    def block_copy(offset):
        return pltpu.make_async_remote_copy(
            src_ref=rows_at(outgoing, offset), dst_ref=rows_at(arrived, offset),
            send_sem=send_sem.at[0], recv_sem=recv_sem.at[offset],
            device_id=partner(offset), device_id_type=MESH)

    def pack(offset, out, parts=(0, 1)):
        base = rows_out[other(offset)]

        def row(k, carry):
            start = base + rows_out[devices + k]
            for part in parts:
                out[block_at(offset, part, k), :] = held[part][pl.ds(start, SUB, stride=SUB), :]
            return carry

        lax.fori_loop(0, share, row, 0, unroll=min(8, share))

    def pack_and_send(seq):
        pack(offset_of(seq), outgoing)
        block_copy(offset_of(seq - 1)).start()

    def sum_copy(kind, offset):
        return pltpu.make_async_remote_copy(
            src_ref=stats.at[kind], dst_ref=totals.at[kind, me],
            send_sem=sum_send.at[kind], recv_sem=sum_recv.at[kind],
            device_id=partner(offset), device_id_type=MESH)

    def send_sums(kind, pair):
        for which in range(2):
            stats[kind, pl.ds(which, 1), :] = jnp.sum(pair[which], axis=0, keepdims=True)
        totals[kind, me] = stats[kind]

        @pl.loop(1, devices)
        def _(offset):
            sum_copy(kind, devices - offset).start()

    def summed(kind):
        every = totals.at[kind, pl.ds(0, devices - 1)]
        pltpu.make_async_remote_copy(
            src_ref=every, dst_ref=every, send_sem=sum_send.at[kind], recv_sem=sum_recv.at[kind],
            device_id=partner(1), device_id_type=MESH).wait()
        total = jnp.sum(totals[kind], axis=0)
        sums[pl.ds(2 * kind, 2), :] = total
        return total

    load_second[0].wait()
    pl.semaphore_wait(barrier, devices - 1)
    pack(offset_of(0), outgoing, (0,))
    load_second[1].wait()
    load_first.start()
    half_copy(offset_of(0), 0).start()
    pack(offset_of(0), outgoing, (1,))
    pack(offset_of(1), outgoing)
    half_copy(offset_of(0), 1).start()

    early = devices // 2
    pl.loop(2, early)(pack_and_send)

    load_first.wait()
    chunk = 8 * SUB

    def squares(i, carry):
        at = pl.multiple_of(i * chunk, chunk)
        above = pl.multiple_of(part_rows + i * chunk, chunk)
        ones = [ref[pl.ds(start, chunk), :].reshape(chunk // SUB, SUB, LANE)
                for ref, start in ((first, at), (first, above), (held_re, at), (held_im, at))]
        squared = [jnp.sum(one * one, axis=0) for one in ones]
        return carry[0] + (squared[0] + squared[1]), carry[1] + (squared[2] + squared[3])

    zero = jnp.zeros((SUB, LANE), jnp.float32)
    squared = lax.fori_loop(0, part_rows // chunk, squares, (zero, zero))
    pack_and_send(early)
    send_sums(0, squared)
    pl.loop(early + 1, devices - 1)(pack_and_send)
    pack(0, arrived)
    block_copy(offset_of(devices - 2)).start()

    def dots(offset, carry):
        base = rows_in[other(offset)]

        def row(k, carry):
            real, imag = carry
            start = base + rows_in[devices + k]
            f_re = first[pl.ds(start, SUB, stride=SUB), :]
            f_im = first[pl.ds(start + part_rows, SUB, stride=SUB), :]
            g_re = arrived[block_at(offset, 0, k), :]
            g_im = arrived[block_at(offset, 1, k), :]
            return real + (f_re * g_re + f_im * g_im), imag + (f_re * g_im - f_im * g_re)

        return lax.fori_loop(0, share, row, carry, unroll=min(8, share))

    def arrival_of(seq):
        pair = seq // (2 * narrow_count)
        turn = lax.rem(seq, 2 * narrow_count) // 2
        which = lax.rem(seq, 2)
        far = jnp.where(inner, jnp.where(turn == 1, last, turn - 1), turn)
        mirror = jnp.where(which == 1, wide_count - 1, 0)
        away = jnp.bitwise_xor(2 * pair + lax.rem(me_w, 2), mirror) * narrow_count + far
        return jnp.where(turn == 0, (2 * pair + which) * narrow_count, away)

    def take(seq, carry):
        offset = arrival_of(seq)
        block_copy(offset).wait_recv()
        return dots(offset, carry)

    final = devices - narrow_count
    carry = lax.fori_loop(1, final, take, dots(0, (zero, zero)))
    mean_second = jnp.sum(summed(0)[1:]) / amp_total
    scale = 1.0 / jnp.sqrt(jnp.broadcast_to(mean_second, (SUB, LANE)) + 1e-06)
    send_sums(1, lax.fori_loop(final, devices, take, carry))

    def group(i, carry):
        base = pl.multiple_of(i * (SUB * SUB), SUB * SUB)
        high = back[SUB + i]
        for r in range(SUB):
            start = high + back[r]
            for part in range(2):
                block = arrived[pl.ds(start + part * half, SUB), :]
                held[part][pl.ds(base + r, SUB, stride=SUB), :] = block * scale
        return carry

    lax.fori_loop(0, blocks_dev // SUB, group, 0, unroll=2)
    sent = pl.ds(message, (devices - 1) * message)
    pltpu.make_async_remote_copy(
        src_ref=outgoing.at[sent, :], dst_ref=arrived.at[sent, :],
        send_sem=send_sem.at[0], recv_sem=recv_sem.at[0],
        device_id=partner(1), device_id_type=MESH).wait_send()
    summed(1)


def store(pieces, amp_total, held_re, held_im, sums, out_hbm, intersection_hbm, norms_hbm,
          intersection, norms, out_sem, scalar_sem):
    part_rows = held_re.shape[0]
    piece = part_rows // pieces
    copies = [pltpu.make_async_copy(held.at[pl.ds(at * piece, piece), :],
                                    out_hbm.at[pl.ds(part * part_rows + at * piece, piece), :],
                                    out_sem.at[part * pieces + at])
              for part, held in enumerate((held_re, held_im)) for at in range(pieces)]
    for copy in copies:
        copy.start()
    means = [jnp.broadcast_to(jnp.sum(sums[pl.ds(row, 1), :]) / amp_total, (SUB, LANE)) for row in range(4)]
    both = jnp.sqrt((means[0] + 1e-06) * (means[1] + 1e-06))
    for which in range(2):
        norms[which] = means[which][0, 0]
        intersection[which] = (means[2 + which] / both)[0, 0]
    copies.append(pltpu.make_async_copy(intersection, intersection_hbm, scalar_sem.at[0]))
    copies.append(pltpu.make_async_copy(norms, norms_hbm, scalar_sem.at[1]))
    for copy in copies[-2:]:
        copy.start()
    for copy in copies:
        copy.wait()


def local(first_state, second_state, place_first, place_second):
    blocks_dev = first_state.shape[1]
    block = first_state.shape[2]
    wide_count = lax.axis_size("wide")
    narrow_count = lax.axis_size("narrow")
    devices = wide_count * narrow_count
    share = blocks_dev // devices
    lines = 1 + bits(blocks_dev * devices) - bits(LANE)
    amp_total = float(blocks_dev * devices * block)

    def tiles(state):
        split = state.reshape(2, blocks_dev // SUB, SUB, block // LANE, LANE)
        return split.transpose(0, 1, 3, 2, 4).reshape(2 * blocks_dev * SUB, LANE)

    pieces = 4
    rows = (2 * blocks_dev * SUB, LANE)
    part = (blocks_dev * SUB, LANE)
    any_spec = pl.BlockSpec(memory_space=pl.ANY)
    hbm_spec = pl.BlockSpec(memory_space=pltpu.HBM)
    vmem_spec = pl.BlockSpec(memory_space=pltpu.VMEM)
    held = pl.pallas_call(
        functools.partial(exchange, (wide_count, narrow_count), blocks_dev, share, amp_total),
        out_shape=(pltpu.VMEM(part, jnp.float32), pltpu.VMEM(part, jnp.float32),
                   pltpu.VMEM((SUB, LANE), jnp.float32)),
        in_specs=[hbm_spec] * 4,
        out_specs=(vmem_spec,) * 3,
        scratch_shapes=[pltpu.VMEM(rows, jnp.float32)] * 3 + [
            pltpu.VMEM((2, 2, LANE), jnp.float32),
            pltpu.VMEM((2, devices, 2, LANE), jnp.float32),
            pltpu.SMEM((2, lines, LANE), jnp.int32),
            pltpu.SMEM((devices + share,), jnp.int32),
            pltpu.SMEM((devices + share,), jnp.int32),
            pltpu.SMEM((SUB + blocks_dev // SUB,), jnp.int32),
            pltpu.SemaphoreType.DMA((3,)),
            pltpu.SemaphoreType.DMA((2,)),
            pltpu.SemaphoreType.DMA((1,)),
            pltpu.SemaphoreType.DMA((devices,)),
            pltpu.SemaphoreType.DMA((2,)),
            pltpu.SemaphoreType.DMA((2,)),
        ],
        compiler_params=pltpu.CompilerParams(
            collective_id=0, has_side_effects=True, vmem_limit_bytes=28 << 20),
        name="exchange",
    )(*(pltpu.with_memory_space_constraint(operand, pltpu.HBM) for operand in (
        place_first.reshape(-1, LANE), place_second.reshape(-1, LANE), tiles(first_state), tiles(second_state))))
    aligned, intersection, norms = pl.pallas_call(
        functools.partial(store, pieces, amp_total),
        out_shape=(jax.ShapeDtypeStruct(rows, jnp.float32),
                   jax.ShapeDtypeStruct((2,), jnp.float32),
                   jax.ShapeDtypeStruct((2,), jnp.float32)),
        in_specs=[vmem_spec] * 3,
        out_specs=(any_spec,) * 3,
        scratch_shapes=[
            pltpu.SMEM((2,), jnp.float32),
            pltpu.SMEM((2,), jnp.float32),
            pltpu.SemaphoreType.DMA((2 * pieces,)),
            pltpu.SemaphoreType.DMA((2,)),
        ],
        compiler_params=pltpu.CompilerParams(vmem_limit_bytes=1 << 20),
        name="store",
    )(*held)
    aligned = aligned.reshape(2, blocks_dev // SUB, block // LANE, SUB, LANE)
    aligned = aligned.transpose(0, 1, 3, 2, 4).reshape(2, blocks_dev, block)
    return (aligned, intersection, norms)


def solution(mesh):
    return jax.shard_map(
        local,
        mesh=mesh,
        in_specs=(P(None, ("wide", "narrow"), None), P(None, ("wide", "narrow"), None), P(), P()),
        out_specs=(P(None, ("wide", "narrow"), None), P(), P()),
        check_vma=False,
    )
```

```python
import functools

import jax
import jax.numpy as jnp
from jax import lax
from jax.experimental import pallas as pl
from jax.experimental.pallas import tpu as pltpu
from jax.sharding import PartitionSpec as P

MESH = pl.DeviceIdType.MESH
SUB = 8
LANE = 128


def row_weight(one_hot):
    return jnp.where(one_hot < SUB, one_hot, one_hot * SUB)


def bits(count):
    return count.bit_length() - 1


def table(ref, base, weights, start=0):
    ref[base] = jnp.int32(start)
    for level, weight in enumerate(weights):
        for low in range(1 << level):
            ref[base + (1 << level) + low] = ref[base + low] + weight


def build_out(place_f, place_s, blocks_dev, devices, share, rows_out):
    zero = jnp.int32(0)
    dev_out = [zero] * bits(devices)
    k_out = [zero] * bits(share)
    unit = jnp.int32(1)
    for level in range(bits(blocks_dev * devices)):
        f = place_f(level)
        s = place_s(level)
        f_dev = f >> bits(blocks_dev)
        both = (f_dev == 0) & ((s >> bits(blocks_dev)) == 0)
        weight = row_weight(s)
        for j in range(bits(devices)):
            dev_out[j] = dev_out[j] + jnp.where(f_dev == (1 << j), weight, 0)
        for i in range(bits(share)):
            k_out[i] = k_out[i] + jnp.where(both & (unit == (1 << i)), weight, 0)
        unit = jnp.where(both, unit * 2, unit)
    table(rows_out, 0, dev_out)
    table(rows_out, devices, k_out)


def build_in(place_f, place_s, blocks_dev, devices, me, share, rows_in, back):
    zero = jnp.int32(0)
    dev_in = [zero] * bits(devices)
    k_in = [zero] * bits(share)
    slot_back = [zero] * bits(blocks_dev)
    unit = jnp.int32(1)
    for level in range(bits(blocks_dev * devices)):
        f = place_f(level)
        s_dev = place_s(level) >> bits(blocks_dev)
        both = ((f >> bits(blocks_dev)) == 0) & (s_dev == 0)
        weight = row_weight(f)
        for j in range(bits(devices)):
            dev_in[j] = dev_in[j] + jnp.where(s_dev == (1 << j), weight, 0)
        for i in range(bits(share)):
            k_in[i] = k_in[i] + jnp.where(both & (unit == (1 << i)), weight, 0)
        toward = jnp.where((s_dev & me) == 0, s_dev, -s_dev)
        packed = jnp.where(both, unit * SUB, toward * (2 * share * SUB))
        for p in range(bits(blocks_dev)):
            slot_back[p] = slot_back[p] + jnp.where(f == (1 << p), packed, 0)
        unit = jnp.where(both, unit * 2, unit)
    table(rows_in, 0, dev_in)
    table(rows_in, devices, k_in)
    table(back, 0, slot_back[:bits(SUB)], me * (2 * share * SUB))
    table(back, SUB, slot_back[bits(SUB):])


def exchange(sizes, blocks_dev, share, amp_total, place_first, place_second, first_hbm, second_hbm,
             held_re, held_im, sums,
             first, outgoing, arrived, squares, squares_w, squares_n, stats, totals, powers, rows_out, rows_in, back,
             load_sem, place_sem, send_sem, recv_sem, sum_send, sum_recv, up, down):
    wide_count, narrow_count = sizes
    devices = wide_count * narrow_count
    levels = bits(blocks_dev * devices)
    me_w = lax.axis_index("wide")
    me_n = lax.axis_index("narrow")
    me = me_w * narrow_count + me_n
    part_rows = blocks_dev * SUB
    half = share * SUB
    message = 2 * half
    held = (held_re, held_im)

    def partner(offset):
        return (jnp.bitwise_xor(me_w, offset // narrow_count),
                jnp.bitwise_xor(me_n, lax.rem(offset, narrow_count)))

    def other(offset):
        other_w, other_n = partner(offset)
        return other_w * narrow_count + other_n

    load_second = [pltpu.make_async_copy(second_hbm.at[pl.ds(part * part_rows, part_rows), :], held[part],
                                         load_sem.at[part]) for part in range(2)]
    load_first = pltpu.make_async_copy(first_hbm, first, load_sem.at[2])
    load_second[0].start()
    last = narrow_count - 1
    inner = (me_n != 0) & (me_n != last)
    reach = 1 if narrow_count == 4 else last
    barrier = pltpu.get_barrier_semaphore()
    for plane in reversed(range(narrow_count)):
        there = jnp.bitwise_xor(me_n, plane)

        @pl.when((there <= me_n + reach) & (there >= me_n - reach))
        def _():
            @pl.loop(0, wide_count if plane else wide_count - 1)
            def _(nearer):
                offset = (wide_count - 1 - nearer) * narrow_count + plane
                pl.semaphore_signal(barrier, inc=1, device_id=partner(offset), device_id_type=MESH)

    lines = [0] + [1 << line for line in range(levels - bits(LANE))]
    for which, place in enumerate((place_first, place_second)):
        for at, line in enumerate(lines):
            pltpu.make_async_copy(place.at[pl.ds(line, 1), :], powers.at[which, pl.ds(at, 1), :],
                                  place_sem.at[which]).start()
    load_second[1].start()
    for which, place in enumerate((place_first, place_second)):
        pltpu.make_async_copy(place.at[pl.ds(0, len(lines)), :], powers.at[which], place_sem.at[which]).wait()

    def place_of(which):
        def entry(level):
            if (1 << level) < LANE:
                return powers[which, 0, 1 << level]
            return powers[which, 1 + level - bits(LANE), 0]
        return entry

    build_out(place_of(0), place_of(1), blocks_dev, devices, share, rows_out)
    flip = jnp.where(lax.rem(me_w, 2) == 1, wide_count - 1, 0)

    def swapped(turn):
        mate = jnp.bitwise_xor(turn, 1)
        return jnp.where(mate < last, mate, turn) + 1

    def offset_of(seq):
        group = seq // narrow_count
        turn = lax.rem(seq, narrow_count)
        opening = last - turn
        far = jnp.where(inner, jnp.where(group == 0, opening, swapped(turn)), turn + 1)
        away = jnp.bitwise_xor(group, flip) * narrow_count + far
        return jnp.where(turn < last, away, (group + 1) * narrow_count)

    def rows_at(ref, offset):
        return ref.at[pl.ds(pl.multiple_of(offset * message, message), message), :]

    def block_at(offset, part, k):
        return pl.ds(pl.multiple_of(offset * message + (part * share + k) * SUB, SUB), SUB)

    def half_copy(offset, part):
        at = pl.ds(pl.multiple_of(offset * message + part * half, half), half)
        return pltpu.make_async_remote_copy(
            src_ref=outgoing.at[at, :], dst_ref=arrived.at[at, :],
            send_sem=send_sem.at[0], recv_sem=recv_sem.at[offset],
            device_id=partner(offset), device_id_type=MESH)

    def block_copy(offset):
        return pltpu.make_async_remote_copy(
            src_ref=rows_at(outgoing, offset), dst_ref=rows_at(arrived, offset),
            send_sem=send_sem.at[0], recv_sem=recv_sem.at[offset],
            device_id=partner(offset), device_id_type=MESH)

    def pack(offset, out, parts=(0, 1)):
        base = rows_out[other(offset)]

        def row(k, carry):
            start = base + rows_out[devices + k]
            for part in parts:
                out[block_at(offset, part, k), :] = held[part][pl.ds(start, SUB, stride=SUB), :]
            return carry

        lax.fori_loop(0, share, row, 0, unroll=min(8, share))

    def pack_and_send(seq):
        pack(offset_of(seq), outgoing)
        block_copy(offset_of(seq - 1)).start()

    def sum_copy(at, src, dst, offset):
        return pltpu.make_async_remote_copy(
            src_ref=src, dst_ref=dst, send_sem=sum_send.at[at], recv_sem=sum_recv.at[at],
            device_id=partner(offset), device_id_type=MESH)

    def keep(ref, pair):
        for which in range(2):
            ref[pl.ds(which, 1), :] = jnp.sum(pair[which], axis=0, keepdims=True)

    def wait_sums(at, ref):
        every = ref.at[pl.ds(0, ref.shape[0] - 1)]
        sum_copy(at, every, every, 1).wait()
        return jnp.sum(ref[...], axis=0)

    def squares_along_wide(pair):
        keep(squares, pair)
        squares_w[me_w] = squares[...]

        @pl.loop(1, wide_count)
        def _(away):
            sum_copy(0, squares, squares_w.at[me_w], away * narrow_count).start()

    def squares_along_narrow():
        total = wait_sums(0, squares_w)
        squares[...] = total
        squares_n[me_n] = squares[...]

        @pl.loop(1, narrow_count)
        def _(plane):
            sum_copy(1, squares, squares_n.at[me_n], plane).start()

    def send_sums(pair):
        keep(stats, pair)
        totals[me] = stats[...]

        for offset in reversed(range(1, devices)):
            sum_copy(2, stats, totals.at[me], offset).start()

    load_second[0].wait()
    planes = jnp.minimum(me_n + reach, last) - jnp.maximum(me_n - reach, 0) + 1
    pl.semaphore_wait(barrier, planes * wide_count - 1)
    pack(offset_of(0), outgoing, (0,))
    half_copy(offset_of(0), 0).start()
    load_second[1].wait()
    load_first.start()
    pack(offset_of(0), outgoing, (1,))
    half_copy(offset_of(0), 1).start()
    if reach < last:
        above = me_n < last - 1
        below = me_n > 1

        def tell(sem, step):
            pl.semaphore_signal(sem, inc=1, device_id=(me_w, me_n + step), device_id_type=MESH)

        pl.when(inner & ~below)(lambda: tell(up, 1))
        pl.when(inner & ~above)(lambda: tell(down, -1))
        pl.when(above)(lambda: pl.semaphore_wait(down, 1))
        pl.when(inner & above)(lambda: tell(down, -1))
        pl.when(below)(lambda: pl.semaphore_wait(up, 1))
        pl.when(inner & below)(lambda: tell(up, 1))
    pack(offset_of(1), outgoing)

    early = 6
    held_back = devices - 3
    pl.loop(2, early)(pack_and_send)
    build_in(place_of(0), place_of(1), blocks_dev, devices, me, share, rows_in, back)

    load_first.wait()
    chunk = 8 * SUB

    def square(i, carry):
        at = pl.multiple_of(i * chunk, chunk)
        above = pl.multiple_of(part_rows + i * chunk, chunk)
        ones = [ref[pl.ds(start, chunk), :].reshape(chunk // SUB, SUB, LANE)
                for ref, start in ((first, at), (first, above), (held_re, at), (held_im, at))]
        squared = [jnp.sum(one * one, axis=0) for one in ones]
        return carry[0] + (squared[0] + squared[1]), carry[1] + (squared[2] + squared[3])

    zero = jnp.zeros((SUB, LANE), jnp.float32)
    squared = lax.fori_loop(0, part_rows // chunk, square, (zero, zero))
    pack_and_send(early)
    squares_along_wide(squared)
    pl.loop(early + 1, held_back + 1)(pack_and_send)

    @pl.loop(held_back + 1, devices - 1)
    def _(seq):
        pack(offset_of(seq), outgoing)

    pack(0, arrived)

    def dots(offset, carry):
        base = rows_in[other(offset)]

        def row(k, carry):
            real, imag = carry
            start = base + rows_in[devices + k]
            f_re = first[pl.ds(start, SUB, stride=SUB), :]
            f_im = first[pl.ds(start + part_rows, SUB, stride=SUB), :]
            g_re = arrived[block_at(offset, 0, k), :]
            g_im = arrived[block_at(offset, 1, k), :]
            return real + (f_re * g_re + f_im * g_im), imag + (f_re * g_im - f_im * g_re)

        return lax.fori_loop(0, share, row, carry, unroll=min(8, share))

    def arrival_of(seq):
        pair = seq // (2 * narrow_count)
        turn = lax.rem(seq, 2 * narrow_count) // 2
        which = lax.rem(seq, 2)
        far = jnp.where(inner, turn, swapped(turn - 1))
        mirror = jnp.where(which == 1, wide_count - 1, 0)
        away = jnp.bitwise_xor(2 * pair + lax.rem(me_w, 2), mirror) * narrow_count + far
        return jnp.where(turn == 0, (2 * pair + which) * narrow_count, away)

    def take(seq, carry):
        offset = arrival_of(seq)
        block_copy(offset).wait_recv()
        return dots(offset, carry)

    middle = devices // 2 - narrow_count
    final = devices - narrow_count
    carry = lax.fori_loop(1, middle, take, dots(0, (zero, zero)))
    squares_along_narrow()

    @pl.loop(held_back, devices - 1)
    def _(seq):
        block_copy(offset_of(seq)).start()

    carry = lax.fori_loop(middle, final, take, carry)
    total = wait_sums(1, squares_n)
    sums[pl.ds(0, 2), :] = total
    mean_second = jnp.sum(total[1:]) / amp_total
    scale = 1.0 / jnp.sqrt(jnp.broadcast_to(mean_second, (SUB, LANE)) + 1e-06)
    send_sums(lax.fori_loop(final, devices, take, carry))

    def group(i, carry):
        base = pl.multiple_of(i * (SUB * SUB), SUB * SUB)
        high = back[SUB + i]
        for r in range(SUB):
            start = high + back[r]
            for part in range(2):
                block = arrived[pl.ds(start + part * half, SUB), :]
                held[part][pl.ds(base + r, SUB, stride=SUB), :] = block * scale
        return carry

    lax.fori_loop(0, blocks_dev // SUB, group, 0, unroll=2)
    sent = pl.ds(message, (devices - 1) * message)
    pltpu.make_async_remote_copy(
        src_ref=outgoing.at[sent, :], dst_ref=arrived.at[sent, :],
        send_sem=send_sem.at[0], recv_sem=recv_sem.at[0],
        device_id=partner(1), device_id_type=MESH).wait_send()
    sums[pl.ds(2, 2), :] = wait_sums(2, totals)


def store(pieces, amp_total, held_re, held_im, sums, out_hbm, intersection_hbm, norms_hbm,
          intersection, norms, out_sem, scalar_sem):
    part_rows = held_re.shape[0]
    piece = part_rows // pieces
    copies = [pltpu.make_async_copy(held.at[pl.ds(at * piece, piece), :],
                                    out_hbm.at[pl.ds(part * part_rows + at * piece, piece), :],
                                    out_sem.at[part * pieces + at])
              for part, held in enumerate((held_re, held_im)) for at in range(pieces)]
    for copy in copies:
        copy.start()
    means = [jnp.broadcast_to(jnp.sum(sums[pl.ds(row, 1), :]) / amp_total, (SUB, LANE)) for row in range(4)]
    both = jnp.sqrt((means[0] + 1e-06) * (means[1] + 1e-06))
    for which in range(2):
        norms[which] = means[which][0, 0]
        intersection[which] = (means[2 + which] / both)[0, 0]
    copies.append(pltpu.make_async_copy(intersection, intersection_hbm, scalar_sem.at[0]))
    copies.append(pltpu.make_async_copy(norms, norms_hbm, scalar_sem.at[1]))
    for copy in copies[-2:]:
        copy.start()
    for copy in copies:
        copy.wait()


def local(first_state, second_state, place_first, place_second):
    blocks_dev = first_state.shape[1]
    block = first_state.shape[2]
    wide_count = lax.axis_size("wide")
    narrow_count = lax.axis_size("narrow")
    devices = wide_count * narrow_count
    share = blocks_dev // devices
    lines = 1 + bits(blocks_dev * devices) - bits(LANE)
    amp_total = float(blocks_dev * devices * block)

    def tiles(state):
        split = state.reshape(2, blocks_dev // SUB, SUB, block // LANE, LANE)
        return split.transpose(0, 1, 3, 2, 4).reshape(2 * blocks_dev * SUB, LANE)

    pieces = 4
    rows = (2 * blocks_dev * SUB, LANE)
    part = (blocks_dev * SUB, LANE)
    any_spec = pl.BlockSpec(memory_space=pl.ANY)
    hbm_spec = pl.BlockSpec(memory_space=pltpu.HBM)
    vmem_spec = pl.BlockSpec(memory_space=pltpu.VMEM)
    held = pl.pallas_call(
        functools.partial(exchange, (wide_count, narrow_count), blocks_dev, share, amp_total),
        out_shape=(pltpu.VMEM(part, jnp.float32), pltpu.VMEM(part, jnp.float32),
                   pltpu.VMEM((SUB, LANE), jnp.float32)),
        in_specs=[hbm_spec] * 4,
        out_specs=(vmem_spec,) * 3,
        scratch_shapes=[pltpu.VMEM(rows, jnp.float32)] * 3 + [
            pltpu.VMEM((2, LANE), jnp.float32),
            pltpu.VMEM((wide_count, 2, LANE), jnp.float32),
            pltpu.VMEM((narrow_count, 2, LANE), jnp.float32),
            pltpu.VMEM((2, LANE), jnp.float32),
            pltpu.VMEM((devices, 2, LANE), jnp.float32),
            pltpu.SMEM((2, lines, LANE), jnp.int32),
            pltpu.SMEM((devices + share,), jnp.int32),
            pltpu.SMEM((devices + share,), jnp.int32),
            pltpu.SMEM((SUB + blocks_dev // SUB,), jnp.int32),
            pltpu.SemaphoreType.DMA((3,)),
            pltpu.SemaphoreType.DMA((2,)),
            pltpu.SemaphoreType.DMA((1,)),
            pltpu.SemaphoreType.DMA((devices,)),
            pltpu.SemaphoreType.DMA((3,)),
            pltpu.SemaphoreType.DMA((3,)),
            pltpu.SemaphoreType.REGULAR,
            pltpu.SemaphoreType.REGULAR,
        ],
        compiler_params=pltpu.CompilerParams(
            collective_id=0, has_side_effects=True, vmem_limit_bytes=28 << 20),
        name="exchange",
    )(*(pltpu.with_memory_space_constraint(operand, pltpu.HBM) for operand in (
        place_first.reshape(-1, LANE), place_second.reshape(-1, LANE), tiles(first_state), tiles(second_state))))
    aligned, intersection, norms = pl.pallas_call(
        functools.partial(store, pieces, amp_total),
        out_shape=(jax.ShapeDtypeStruct(rows, jnp.float32),
                   jax.ShapeDtypeStruct((2,), jnp.float32),
                   jax.ShapeDtypeStruct((2,), jnp.float32)),
        in_specs=[vmem_spec] * 3,
        out_specs=(any_spec,) * 3,
        scratch_shapes=[
            pltpu.SMEM((2,), jnp.float32),
            pltpu.SMEM((2,), jnp.float32),
            pltpu.SemaphoreType.DMA((2 * pieces,)),
            pltpu.SemaphoreType.DMA((2,)),
        ],
        compiler_params=pltpu.CompilerParams(vmem_limit_bytes=1 << 20),
        name="store",
    )(*held)
    aligned = aligned.reshape(2, blocks_dev // SUB, block // LANE, SUB, LANE)
    aligned = aligned.transpose(0, 1, 3, 2, 4).reshape(2, blocks_dev, block)
    return (aligned, intersection, norms)


def solution(mesh):
    return jax.shard_map(
        local,
        mesh=mesh,
        in_specs=(P(None, ("wide", "narrow"), None), P(None, ("wide", "narrow"), None), P(), P()),
        out_specs=(P(None, ("wide", "narrow"), None), P(), P()),
        check_vma=False,
    )
```

```python
import functools

import jax
import jax.numpy as jnp
from jax import lax
from jax.experimental import pallas as pl
from jax.experimental.pallas import tpu as pltpu
from jax.sharding import PartitionSpec as P

MESH = pl.DeviceIdType.MESH
SUB = 8
LANE = 128


def row_weight(one_hot):
    return jnp.where(one_hot < SUB, one_hot, one_hot * SUB)


def bits(count):
    return count.bit_length() - 1


def table(ref, base, weights, start=0):
    ref[base] = jnp.int32(start)
    for level, weight in enumerate(weights):
        for low in range(1 << level):
            ref[base + (1 << level) + low] = ref[base + low] + weight


def build_out(place_f, place_s, blocks_dev, devices, share, rows_out):
    zero = jnp.int32(0)
    dev_out = [zero] * bits(devices)
    k_out = [zero] * bits(share)
    unit = jnp.int32(1)
    for level in range(bits(blocks_dev * devices)):
        f = place_f(level)
        s = place_s(level)
        f_dev = f >> bits(blocks_dev)
        both = (f_dev == 0) & ((s >> bits(blocks_dev)) == 0)
        weight = row_weight(s)
        for j in range(bits(devices)):
            dev_out[j] = dev_out[j] + jnp.where(f_dev == (1 << j), weight, 0)
        for i in range(bits(share)):
            k_out[i] = k_out[i] + jnp.where(both & (unit == (1 << i)), weight, 0)
        unit = jnp.where(both, unit * 2, unit)
    table(rows_out, 0, dev_out)
    table(rows_out, devices, k_out)


def build_in(place_f, place_s, blocks_dev, devices, me, share, rows_in, back):
    zero = jnp.int32(0)
    dev_in = [zero] * bits(devices)
    k_in = [zero] * bits(share)
    slot_back = [zero] * bits(blocks_dev)
    unit = jnp.int32(1)
    for level in range(bits(blocks_dev * devices)):
        f = place_f(level)
        s_dev = place_s(level) >> bits(blocks_dev)
        both = ((f >> bits(blocks_dev)) == 0) & (s_dev == 0)
        weight = row_weight(f)
        for j in range(bits(devices)):
            dev_in[j] = dev_in[j] + jnp.where(s_dev == (1 << j), weight, 0)
        for i in range(bits(share)):
            k_in[i] = k_in[i] + jnp.where(both & (unit == (1 << i)), weight, 0)
        toward = jnp.where((s_dev & me) == 0, s_dev, -s_dev)
        packed = jnp.where(both, unit * SUB, toward * (2 * share * SUB))
        for p in range(bits(blocks_dev)):
            slot_back[p] = slot_back[p] + jnp.where(f == (1 << p), packed, 0)
        unit = jnp.where(both, unit * 2, unit)
    table(rows_in, 0, dev_in)
    table(rows_in, devices, k_in)
    table(back, 0, slot_back[:bits(SUB)], me * (2 * share * SUB))
    table(back, SUB, slot_back[bits(SUB):])


def exchange(sizes, blocks_dev, share, amp_total, place_first, place_second, first_hbm, second_hbm,
             held_re, held_im, sums,
             first, outgoing, arrived, ready, squares, squares_w, squares_n, stats, totals, powers, rows_out, rows_in, back,
             load_sem, place_sem, send_sem, recv_sem, sum_send, sum_recv, up, down):
    wide_count, narrow_count = sizes
    devices = wide_count * narrow_count
    levels = bits(blocks_dev * devices)
    me_w = lax.axis_index("wide")
    me_n = lax.axis_index("narrow")
    me = me_w * narrow_count + me_n
    part_rows = blocks_dev * SUB
    half = share * SUB
    message = 2 * half
    held = (held_re, held_im)

    def partner(offset):
        return (jnp.bitwise_xor(me_w, offset // narrow_count),
                jnp.bitwise_xor(me_n, lax.rem(offset, narrow_count)))

    def other(offset):
        other_w, other_n = partner(offset)
        return other_w * narrow_count + other_n

    load_second = [pltpu.make_async_copy(second_hbm.at[pl.ds(part * part_rows, part_rows), :], held[part],
                                         load_sem.at[part]) for part in range(2)]
    load_first = pltpu.make_async_copy(first_hbm, first, load_sem.at[2])
    load_second[0].start()
    last = narrow_count - 1
    inner = (me_n != 0) & (me_n != last)
    reach = 1 if narrow_count == 4 else last
    barrier = pltpu.get_barrier_semaphore()
    for plane in reversed(range(narrow_count)):
        there = jnp.bitwise_xor(me_n, plane)

        @pl.when((there <= me_n + reach) & (there >= me_n - reach))
        def _():
            @pl.loop(0, wide_count if plane else wide_count - 1)
            def _(nearer):
                offset = (wide_count - 1 - nearer) * narrow_count + plane
                pl.semaphore_signal(barrier, inc=1, device_id=partner(offset), device_id_type=MESH)

    lines = [0] + [1 << line for line in range(levels - bits(LANE))]
    for which, place in enumerate((place_first, place_second)):
        for at, line in enumerate(lines):
            pltpu.make_async_copy(place.at[pl.ds(line, 1), :], powers.at[which, pl.ds(at, 1), :],
                                  place_sem.at[which]).start()
    load_second[1].start()
    for which, place in enumerate((place_first, place_second)):
        pltpu.make_async_copy(place.at[pl.ds(0, len(lines)), :], powers.at[which], place_sem.at[which]).wait()

    def place_of(which):
        def entry(level):
            if (1 << level) < LANE:
                return powers[which, 0, 1 << level]
            return powers[which, 1 + level - bits(LANE), 0]
        return entry

    build_out(place_of(0), place_of(1), blocks_dev, devices, share, rows_out)
    flip = jnp.where(lax.rem(me_w, 2) == 1, wide_count - 1, 0)

    def swapped(turn):
        mate = jnp.bitwise_xor(turn, 1)
        return jnp.where(mate < last, mate, turn) + 1

    def offset_of(seq):
        group = seq // narrow_count
        turn = lax.rem(seq, narrow_count)
        opening = last - turn
        far = jnp.where(inner, jnp.where(group == 0, opening, swapped(turn)), turn + 1)
        away = jnp.bitwise_xor(group, flip) * narrow_count + far
        return jnp.where(turn < last, away, (group + 1) * narrow_count)

    def rows_at(ref, offset):
        return ref.at[pl.ds(pl.multiple_of(offset * message, message), message), :]

    def block_at(offset, part, k):
        return pl.ds(pl.multiple_of(offset * message + (part * share + k) * SUB, SUB), SUB)

    def half_copy(offset, part):
        at = pl.ds(pl.multiple_of(offset * message + part * half, half), half)
        return pltpu.make_async_remote_copy(
            src_ref=outgoing.at[at, :], dst_ref=arrived.at[at, :],
            send_sem=send_sem.at[0], recv_sem=recv_sem.at[offset],
            device_id=partner(offset), device_id_type=MESH)

    def block_copy(offset):
        return pltpu.make_async_remote_copy(
            src_ref=rows_at(outgoing, offset), dst_ref=rows_at(arrived, offset),
            send_sem=send_sem.at[0], recv_sem=recv_sem.at[offset],
            device_id=partner(offset), device_id_type=MESH)

    def pack(offset, out, parts=(0, 1)):
        base = rows_out[other(offset)]

        def row(k, carry):
            start = base + rows_out[devices + k]
            for part in parts:
                out[block_at(offset, part, k), :] = held[part][pl.ds(start, SUB, stride=SUB), :]
            return carry

        lax.fori_loop(0, share, row, 0, unroll=min(8, share))

    def pack_and_send(seq):
        pack(offset_of(seq), outgoing)
        block_copy(offset_of(seq - 1)).start()

    def sum_copy(at, src, dst, offset):
        return pltpu.make_async_remote_copy(
            src_ref=src, dst_ref=dst, send_sem=sum_send.at[at], recv_sem=sum_recv.at[at],
            device_id=partner(offset), device_id_type=MESH)

    def keep(ref, pair):
        for which in range(2):
            ref[pl.ds(which, 1), :] = jnp.sum(pair[which], axis=0, keepdims=True)

    def wait_sums(at, ref):
        every = ref.at[pl.ds(0, ref.shape[0] - 1)]
        sum_copy(at, every, every, 1).wait()
        return jnp.sum(ref[...], axis=0)

    def squares_along_wide(pair):
        keep(squares, pair)
        squares_w[me_w] = squares[...]

        @pl.loop(1, wide_count)
        def _(away):
            sum_copy(0, squares, squares_w.at[me_w], away * narrow_count).start()

    def squares_along_narrow():
        total = wait_sums(0, squares_w)
        squares[...] = total
        squares_n[me_n] = squares[...]

        @pl.loop(1, narrow_count)
        def _(plane):
            sum_copy(1, squares, squares_n.at[me_n], plane).start()

    def send_sums(pair):
        folded = [one + pltpu.roll(one, LANE // 2, 1) for one in pair]
        lane = lax.broadcasted_iota(jnp.int32, (SUB, LANE), 1)
        stats[...] = jnp.sum(jnp.where(lane < LANE // 2, folded[0], folded[1]), axis=0, keepdims=True)
        totals[me] = stats[...]

        for offset in reversed(range(1, devices)):
            sum_copy(2, stats, totals.at[me], offset).start()

    load_second[0].wait()
    planes = jnp.minimum(me_n + reach, last) - jnp.maximum(me_n - reach, 0) + 1
    pl.semaphore_wait(barrier, planes * wide_count - 1)
    pack(offset_of(0), outgoing, (0,))
    half_copy(offset_of(0), 0).start()
    load_second[1].wait()
    load_first.start()
    pack(offset_of(0), outgoing, (1,))
    half_copy(offset_of(0), 1).start()
    if reach < last:
        above = me_n < last - 1
        below = me_n > 1

        def tell(sem, step):
            pl.semaphore_signal(sem, inc=1, device_id=(me_w, me_n + step), device_id_type=MESH)

        pl.when(inner & ~below)(lambda: tell(up, 1))
        pl.when(inner & ~above)(lambda: tell(down, -1))
        pl.when(above)(lambda: pl.semaphore_wait(down, 1))
        pl.when(inner & above)(lambda: tell(down, -1))
        pl.when(below)(lambda: pl.semaphore_wait(up, 1))
        pl.when(inner & below)(lambda: tell(up, 1))
    pack(offset_of(1), outgoing)

    early = 6
    held_back = devices - 3
    pl.loop(2, early)(pack_and_send)
    build_in(place_of(0), place_of(1), blocks_dev, devices, me, share, rows_in, back)

    load_first.wait()
    chunk = 8 * SUB

    def square(i, carry):
        at = pl.multiple_of(i * chunk, chunk)
        above = pl.multiple_of(part_rows + i * chunk, chunk)
        ones = [ref[pl.ds(start, chunk), :].reshape(chunk // SUB, SUB, LANE)
                for ref, start in ((first, at), (first, above), (held_re, at), (held_im, at))]
        squared = [jnp.sum(one * one, axis=0) for one in ones]
        return carry[0] + (squared[0] + squared[1]), carry[1] + (squared[2] + squared[3])

    zero = jnp.zeros((SUB, LANE), jnp.float32)
    squared = lax.fori_loop(0, part_rows // chunk, square, (zero, zero))
    pack_and_send(early)
    squares_along_wide(squared)
    pl.loop(early + 1, held_back + 1)(pack_and_send)

    @pl.loop(held_back + 1, devices - 1)
    def _(seq):
        pack(offset_of(seq), outgoing)

    pack(0, arrived)

    def dots(offset, carry):
        base = rows_in[other(offset)]

        def row(k, carry):
            real, imag = carry
            start = base + rows_in[devices + k]
            f_re = first[pl.ds(start, SUB, stride=SUB), :]
            f_im = first[pl.ds(start + part_rows, SUB, stride=SUB), :]
            g_re = arrived[block_at(offset, 0, k), :]
            g_im = arrived[block_at(offset, 1, k), :]
            return real + (f_re * g_re + f_im * g_im), imag + (f_re * g_im - f_im * g_re)

        return lax.fori_loop(0, share, row, carry, unroll=min(8, share))

    def dots_ready(slot, offset, carry):
        def row(k, carry):
            real, imag = carry
            f_re, f_im = (ready[block_at(slot, part, k), :] for part in range(2))
            g_re, g_im = (arrived[block_at(offset, part, k), :] for part in range(2))
            return real + (f_re * g_re + f_im * g_im), imag + (f_re * g_im - f_im * g_re)

        return lax.fori_loop(0, share, row, carry, unroll=min(16, share))

    def make_ready(seq, slot):
        base = rows_in[other(arrival_of(seq))]

        def row(k, carry):
            start = base + rows_in[devices + k]
            for part in range(2):
                ready[block_at(slot, part, k), :] = first[pl.ds(start + part * part_rows, SUB, stride=SUB), :]
            return carry

        lax.fori_loop(0, share, row, 0, unroll=min(8, share))

    def arrival_of(seq):
        pair = seq // (2 * narrow_count)
        turn = lax.rem(seq, 2 * narrow_count) // 2
        which = lax.rem(seq, 2)
        far = jnp.where(inner, turn, swapped(turn - 1))
        mirror = jnp.where(which == 1, wide_count - 1, 0)
        away = jnp.bitwise_xor(2 * pair + lax.rem(me_w, 2), mirror) * narrow_count + far
        return jnp.where(turn == 0, (2 * pair + which) * narrow_count, away)

    def take(seq, carry):
        offset = arrival_of(seq)
        block_copy(offset).wait_recv()
        return dots(offset, carry)

    def take_ready(seq, carry):
        offset = arrival_of(seq)
        block_copy(offset).wait_recv()
        return dots_ready(seq - final, offset, carry)

    middle = devices // 2 - narrow_count
    final = devices - narrow_count
    carry = lax.fori_loop(1, middle, take, dots(0, (zero, zero)))
    squares_along_narrow()

    @pl.loop(held_back, devices - 1)
    def _(seq):
        block_copy(offset_of(seq)).start()

    @pl.loop(final, devices)
    def _(seq):
        make_ready(seq, seq - final)

    carry = lax.fori_loop(middle, final, take, carry)
    total = wait_sums(1, squares_n)
    sums[pl.ds(0, 2), :] = total
    mean_second = jnp.sum(total[1:]) / amp_total
    scale = 1.0 / jnp.sqrt(jnp.broadcast_to(mean_second, (SUB, LANE)) + 1e-06)
    send_sums(lax.fori_loop(final, devices, take_ready, carry))

    def group(i, carry):
        base = pl.multiple_of(i * (SUB * SUB), SUB * SUB)
        high = back[SUB + i]
        for r in range(SUB):
            start = high + back[r]
            for part in range(2):
                block = arrived[pl.ds(start + part * half, SUB), :]
                held[part][pl.ds(base + r, SUB, stride=SUB), :] = block * scale
        return carry

    lax.fori_loop(0, blocks_dev // SUB, group, 0, unroll=2)
    sent = pl.ds(message, (devices - 1) * message)
    pltpu.make_async_remote_copy(
        src_ref=outgoing.at[sent, :], dst_ref=arrived.at[sent, :],
        send_sem=send_sem.at[0], recv_sem=recv_sem.at[0],
        device_id=partner(1), device_id_type=MESH).wait_send()
    sums[pl.ds(2, 1), :] = wait_sums(2, totals)


def store(pieces, amp_total, held_re, held_im, sums, out_hbm, intersection_hbm, norms_hbm,
          intersection, norms, out_sem, scalar_sem):
    part_rows = held_re.shape[0]
    piece = part_rows // pieces
    copies = [pltpu.make_async_copy(held.at[pl.ds(at * piece, piece), :],
                                    out_hbm.at[pl.ds(part * part_rows + at * piece, piece), :],
                                    out_sem.at[part * pieces + at])
              for part, held in enumerate((held_re, held_im)) for at in range(pieces)]
    for copy in copies:
        copy.start()
    low = lax.broadcasted_iota(jnp.int32, (1, LANE), 1) < LANE // 2
    dots = sums[pl.ds(2, 1), :]
    parts = (sums[pl.ds(0, 1), :], sums[pl.ds(1, 1), :], jnp.where(low, dots, 0.0), jnp.where(low, 0.0, dots))
    means = [jnp.broadcast_to(jnp.sum(one) / amp_total, (SUB, LANE)) for one in parts]
    both = jnp.sqrt((means[0] + 1e-06) * (means[1] + 1e-06))
    for which in range(2):
        norms[which] = means[which][0, 0]
        intersection[which] = (means[2 + which] / both)[0, 0]
    copies.append(pltpu.make_async_copy(intersection, intersection_hbm, scalar_sem.at[0]))
    copies.append(pltpu.make_async_copy(norms, norms_hbm, scalar_sem.at[1]))
    for copy in copies[-2:]:
        copy.start()
    for copy in copies:
        copy.wait()


def local(first_state, second_state, place_first, place_second):
    blocks_dev = first_state.shape[1]
    block = first_state.shape[2]
    wide_count = lax.axis_size("wide")
    narrow_count = lax.axis_size("narrow")
    devices = wide_count * narrow_count
    share = blocks_dev // devices
    lines = 1 + bits(blocks_dev * devices) - bits(LANE)
    amp_total = float(blocks_dev * devices * block)

    def tiles(state):
        split = state.reshape(2, blocks_dev // SUB, SUB, block // LANE, LANE)
        return split.transpose(0, 1, 3, 2, 4).reshape(2 * blocks_dev * SUB, LANE)

    pieces = 4
    rows = (2 * blocks_dev * SUB, LANE)
    part = (blocks_dev * SUB, LANE)
    any_spec = pl.BlockSpec(memory_space=pl.ANY)
    hbm_spec = pl.BlockSpec(memory_space=pltpu.HBM)
    vmem_spec = pl.BlockSpec(memory_space=pltpu.VMEM)
    held = pl.pallas_call(
        functools.partial(exchange, (wide_count, narrow_count), blocks_dev, share, amp_total),
        out_shape=(pltpu.VMEM(part, jnp.float32), pltpu.VMEM(part, jnp.float32),
                   pltpu.VMEM((SUB, LANE), jnp.float32)),
        in_specs=[hbm_spec] * 4,
        out_specs=(vmem_spec,) * 3,
        scratch_shapes=[pltpu.VMEM(rows, jnp.float32)] * 3 + [
            pltpu.VMEM((narrow_count * 2 * share * SUB, LANE), jnp.float32),
            pltpu.VMEM((2, LANE), jnp.float32),
            pltpu.VMEM((wide_count, 2, LANE), jnp.float32),
            pltpu.VMEM((narrow_count, 2, LANE), jnp.float32),
            pltpu.VMEM((1, LANE), jnp.float32),
            pltpu.VMEM((devices, 1, LANE), jnp.float32),
            pltpu.SMEM((2, lines, LANE), jnp.int32),
            pltpu.SMEM((devices + share,), jnp.int32),
            pltpu.SMEM((devices + share,), jnp.int32),
            pltpu.SMEM((SUB + blocks_dev // SUB,), jnp.int32),
            pltpu.SemaphoreType.DMA((3,)),
            pltpu.SemaphoreType.DMA((2,)),
            pltpu.SemaphoreType.DMA((1,)),
            pltpu.SemaphoreType.DMA((devices,)),
            pltpu.SemaphoreType.DMA((3,)),
            pltpu.SemaphoreType.DMA((3,)),
            pltpu.SemaphoreType.REGULAR,
            pltpu.SemaphoreType.REGULAR,
        ],
        compiler_params=pltpu.CompilerParams(
            collective_id=0, has_side_effects=True, vmem_limit_bytes=28 << 20),
        name="exchange",
    )(*(pltpu.with_memory_space_constraint(operand, pltpu.HBM) for operand in (
        place_first.reshape(-1, LANE), place_second.reshape(-1, LANE), tiles(first_state), tiles(second_state))))
    aligned, intersection, norms = pl.pallas_call(
        functools.partial(store, pieces, amp_total),
        out_shape=(jax.ShapeDtypeStruct(rows, jnp.float32),
                   jax.ShapeDtypeStruct((2,), jnp.float32),
                   jax.ShapeDtypeStruct((2,), jnp.float32)),
        in_specs=[vmem_spec] * 3,
        out_specs=(any_spec,) * 3,
        scratch_shapes=[
            pltpu.SMEM((2,), jnp.float32),
            pltpu.SMEM((2,), jnp.float32),
            pltpu.SemaphoreType.DMA((2 * pieces,)),
            pltpu.SemaphoreType.DMA((2,)),
        ],
        compiler_params=pltpu.CompilerParams(vmem_limit_bytes=1 << 20),
        name="store",
    )(*held)
    aligned = aligned.reshape(2, blocks_dev // SUB, block // LANE, SUB, LANE)
    aligned = aligned.transpose(0, 1, 3, 2, 4).reshape(2, blocks_dev, block)
    return (aligned, intersection, norms)


def solution(mesh):
    return jax.shard_map(
        local,
        mesh=mesh,
        in_specs=(P(None, ("wide", "narrow"), None), P(None, ("wide", "narrow"), None), P(), P()),
        out_specs=(P(None, ("wide", "narrow"), None), P(), P()),
        check_vma=False,
    )
```

```python
import functools

import jax
import jax.numpy as jnp
from jax import lax
from jax.experimental import pallas as pl
from jax.experimental.pallas import tpu as pltpu
from jax.sharding import PartitionSpec as P

MESH = pl.DeviceIdType.MESH
SUB = 8
LANE = 128


def row_weight(one_hot):
    return jnp.where(one_hot < SUB, one_hot, one_hot * SUB)


def bits(count):
    return count.bit_length() - 1


def table(ref, base, weights, start=0):
    ref[base] = jnp.int32(start)
    for level, weight in enumerate(weights):
        for low in range(1 << level):
            ref[base + (1 << level) + low] = ref[base + low] + weight


def build_out(place_f, place_s, blocks_dev, devices, share, rows_out):
    zero = jnp.int32(0)
    dev_out = [zero] * bits(devices)
    k_out = [zero] * bits(share)
    unit = jnp.int32(1)
    for level in range(bits(blocks_dev * devices)):
        f = place_f(level)
        s = place_s(level)
        f_dev = f >> bits(blocks_dev)
        both = (f_dev == 0) & ((s >> bits(blocks_dev)) == 0)
        weight = row_weight(s)
        for j in range(bits(devices)):
            dev_out[j] = dev_out[j] + jnp.where(f_dev == (1 << j), weight, 0)
        for i in range(bits(share)):
            k_out[i] = k_out[i] + jnp.where(both & (unit == (1 << i)), weight, 0)
        unit = jnp.where(both, unit * 2, unit)
    table(rows_out, 0, dev_out)
    table(rows_out, devices, k_out)


def build_in(place_f, place_s, blocks_dev, devices, me, share, rows_in, back):
    zero = jnp.int32(0)
    dev_in = [zero] * bits(devices)
    k_in = [zero] * bits(share)
    slot_back = [zero] * bits(blocks_dev)
    unit = jnp.int32(1)
    for level in range(bits(blocks_dev * devices)):
        f = place_f(level)
        s_dev = place_s(level) >> bits(blocks_dev)
        both = ((f >> bits(blocks_dev)) == 0) & (s_dev == 0)
        weight = row_weight(f)
        for j in range(bits(devices)):
            dev_in[j] = dev_in[j] + jnp.where(s_dev == (1 << j), weight, 0)
        for i in range(bits(share)):
            k_in[i] = k_in[i] + jnp.where(both & (unit == (1 << i)), weight, 0)
        toward = jnp.where((s_dev & me) == 0, s_dev, -s_dev)
        packed = jnp.where(both, unit * SUB, toward * (2 * share * SUB))
        for p in range(bits(blocks_dev)):
            slot_back[p] = slot_back[p] + jnp.where(f == (1 << p), packed, 0)
        unit = jnp.where(both, unit * 2, unit)
    table(rows_in, 0, dev_in)
    table(rows_in, devices, k_in)
    table(back, 0, slot_back[:bits(SUB)], me * (2 * share * SUB))
    table(back, SUB, slot_back[bits(SUB):])


def exchange(sizes, blocks_dev, share, amp_total, place_first, place_second, first_hbm, second_hbm,
             held_re, held_im, sums,
             first, outgoing, arrived, ready, squares, squares_w, squares_n, stats, totals, powers, rows_out, rows_in, back,
             load_sem, place_sem, send_sem, recv_sem, sum_send, sum_recv, known):
    wide_count, narrow_count = sizes
    devices = wide_count * narrow_count
    levels = bits(blocks_dev * devices)
    me_w = lax.axis_index("wide")
    me_n = lax.axis_index("narrow")
    me = me_w * narrow_count + me_n
    part_rows = blocks_dev * SUB
    half = share * SUB
    message = 2 * half
    held = (held_re, held_im)

    def partner(offset):
        return (jnp.bitwise_xor(me_w, offset // narrow_count),
                jnp.bitwise_xor(me_n, lax.rem(offset, narrow_count)))

    def other(offset):
        other_w, other_n = partner(offset)
        return other_w * narrow_count + other_n

    load_second = [pltpu.make_async_copy(second_hbm.at[pl.ds(part * part_rows, part_rows), :], held[part],
                                         load_sem.at[part]) for part in range(2)]
    load_first = pltpu.make_async_copy(first_hbm, first, load_sem.at[2])
    load_second[0].start()
    last = narrow_count - 1
    inner = (me_n != 0) & (me_n != last)
    chained = narrow_count == 4
    barrier = pltpu.get_barrier_semaphore()

    def greet(where_w, where_n):
        pl.semaphore_signal(barrier, inc=1, device_id=(where_w, where_n), device_id_type=MESH)

    if chained:
        for step in (-1, 1, 0):
            there = me_n + step

            @pl.when((there > 0) & (there < last))
            def _():
                for mate in ((0, 1) if step else (1,)):
                    greet(jnp.bitwise_xor(me_w, mate), there)

        for end in (0, last):
            @pl.loop(1, wide_count)
            def _(away):
                greet(jnp.bitwise_xor(me_w, wide_count - away), end)

            pl.when(me_n != end)(lambda: greet(me_w, end))
    else:
        @pl.loop(1, devices)
        def _(offset):
            greet(*partner(offset))

    greeted = jnp.where(inner, 5, devices - 1) if chained else devices - 1

    lines = [0] + [1 << line for line in range(levels - bits(LANE))]
    for which, place in enumerate((place_first, place_second)):
        for at, line in enumerate(lines):
            pltpu.make_async_copy(place.at[pl.ds(line, 1), :], powers.at[which, pl.ds(at, 1), :],
                                  place_sem.at[which]).start()
    load_second[1].start()
    for which, place in enumerate((place_first, place_second)):
        pltpu.make_async_copy(place.at[pl.ds(0, len(lines)), :], powers.at[which], place_sem.at[which]).wait()

    def place_of(which):
        def entry(level):
            if (1 << level) < LANE:
                return powers[which, 0, 1 << level]
            return powers[which, 1 + level - bits(LANE), 0]
        return entry

    build_out(place_of(0), place_of(1), blocks_dev, devices, share, rows_out)
    flip = jnp.where(lax.rem(me_w, 2) == 1, wide_count - 1, 0)

    def swapped(turn):
        mate = jnp.bitwise_xor(turn, 1)
        return jnp.where(mate < last, mate, turn) + 1

    odd = lax.rem(me_w, 2) == 1

    def offset_of(seq):
        first_far = jnp.where(inner, last, 1)
        opened = (wide_count - 2) * narrow_count + jnp.where(inner, last - 1, 0)
        later = seq - jnp.where(seq <= opened, 1, 0)
        at = jnp.where(odd, later, seq + jnp.where(seq < last, 0, 1))
        group = at // narrow_count
        turn = lax.rem(at, narrow_count)
        opening = last - turn
        far = jnp.where(inner, jnp.where(group == 0, opening, swapped(turn)), turn + 1)
        away = jnp.bitwise_xor(group, flip) * narrow_count + far
        near = (group + jnp.where(odd, 1, 0)) * narrow_count
        return jnp.where(odd & (seq == 0), narrow_count + first_far, jnp.where(turn < last, away, near))

    def rows_at(ref, offset):
        return ref.at[pl.ds(pl.multiple_of(offset * message, message), message), :]

    def block_at(offset, part, k):
        return pl.ds(pl.multiple_of(offset * message + (part * share + k) * SUB, SUB), SUB)

    def half_copy(offset, part):
        at = pl.ds(pl.multiple_of(offset * message + part * half, half), half)
        return pltpu.make_async_remote_copy(
            src_ref=outgoing.at[at, :], dst_ref=arrived.at[at, :],
            send_sem=send_sem.at[0], recv_sem=recv_sem.at[offset],
            device_id=partner(offset), device_id_type=MESH)

    def block_copy(offset):
        return pltpu.make_async_remote_copy(
            src_ref=rows_at(outgoing, offset), dst_ref=rows_at(arrived, offset),
            send_sem=send_sem.at[0], recv_sem=recv_sem.at[offset],
            device_id=partner(offset), device_id_type=MESH)

    def pack(offset, out, parts=(0, 1)):
        base = rows_out[other(offset)]

        def row(k, carry):
            start = base + rows_out[devices + k]
            for part in parts:
                out[block_at(offset, part, k), :] = held[part][pl.ds(start, SUB, stride=SUB), :]
            return carry

        lax.fori_loop(0, share, row, 0, unroll=min(8, share))

    def pack_and_send(seq):
        pack(offset_of(seq), outgoing)
        block_copy(offset_of(seq - 1)).start()

    def sum_copy(at, src, dst, offset):
        return pltpu.make_async_remote_copy(
            src_ref=src, dst_ref=dst, send_sem=sum_send.at[at], recv_sem=sum_recv.at[at],
            device_id=partner(offset), device_id_type=MESH)

    def keep(ref, pair):
        for which in range(2):
            ref[pl.ds(which, 1), :] = jnp.sum(pair[which], axis=0, keepdims=True)

    def wait_sums(at, ref):
        every = ref.at[pl.ds(0, ref.shape[0] - 1)]
        sum_copy(at, every, every, 1).wait()
        return jnp.sum(ref[...], axis=0)

    def squares_along_wide(pair):
        keep(squares, pair)
        squares_w[me_w] = squares[...]

        @pl.loop(1, wide_count)
        def _(away):
            sum_copy(0, squares, squares_w.at[me_w], away * narrow_count).start()

    def squares_along_narrow():
        total = wait_sums(0, squares_w)
        squares[...] = total
        squares_n[me_n] = squares[...]

        @pl.loop(1, narrow_count)
        def _(plane):
            sum_copy(1, squares, squares_n.at[me_n], plane).start()

    def send_sums(pair):
        folded = [one + pltpu.roll(one, LANE // 2, 1) for one in pair]
        lane = lax.broadcasted_iota(jnp.int32, (SUB, LANE), 1)
        stats[...] = jnp.sum(jnp.where(lane < LANE // 2, folded[0], folded[1]), axis=0, keepdims=True)
        totals[me] = stats[...]

        for offset in reversed(range(1, devices)):
            sum_copy(2, stats, totals.at[me], offset).start()

    load_second[0].wait()
    pl.semaphore_wait(barrier, greeted)
    pack(offset_of(0), outgoing, (0,))
    half_copy(offset_of(0), 0).start()
    load_second[1].wait()
    load_first.start()
    pack(offset_of(0), outgoing, (1,))
    half_copy(offset_of(0), 1).start()
    if chained:
        pl.when(inner)(lambda: pl.semaphore_wait(known, 1))

        @pl.when(me_n > 1)
        def _():
            pl.semaphore_signal(known, inc=1, device_id=(me_w, me_n - 1), device_id_type=MESH)

    pack(offset_of(1), outgoing)

    early = 6
    held_back = devices - 3
    pl.loop(2, early)(pack_and_send)
    build_in(place_of(0), place_of(1), blocks_dev, devices, me, share, rows_in, back)

    load_first.wait()
    chunk = 8 * SUB

    def square(i, carry):
        at = pl.multiple_of(i * chunk, chunk)
        above = pl.multiple_of(part_rows + i * chunk, chunk)
        ones = [ref[pl.ds(start, chunk), :].reshape(chunk // SUB, SUB, LANE)
                for ref, start in ((first, at), (first, above), (held_re, at), (held_im, at))]
        squared = [jnp.sum(one * one, axis=0) for one in ones]
        return carry[0] + (squared[0] + squared[1]), carry[1] + (squared[2] + squared[3])

    zero = jnp.zeros((SUB, LANE), jnp.float32)
    squared = lax.fori_loop(0, part_rows // chunk, square, (zero, zero))
    pack_and_send(early)
    squares_along_wide(squared)
    pl.loop(early + 1, held_back + 1)(pack_and_send)

    @pl.loop(held_back + 1, devices - 1)
    def _(seq):
        pack(offset_of(seq), outgoing)

    pack(0, arrived)

    def dots(offset, carry):
        base = rows_in[other(offset)]

        def row(k, carry):
            real, imag = carry
            start = base + rows_in[devices + k]
            f_re = first[pl.ds(start, SUB, stride=SUB), :]
            f_im = first[pl.ds(start + part_rows, SUB, stride=SUB), :]
            g_re = arrived[block_at(offset, 0, k), :]
            g_im = arrived[block_at(offset, 1, k), :]
            return real + (f_re * g_re + f_im * g_im), imag + (f_re * g_im - f_im * g_re)

        return lax.fori_loop(0, share, row, carry, unroll=min(8, share))

    def dots_ready(slot, offset, carry):
        def row(k, carry):
            real, imag = carry
            f_re, f_im = (ready[block_at(slot, part, k), :] for part in range(2))
            g_re, g_im = (arrived[block_at(offset, part, k), :] for part in range(2))
            return real + (f_re * g_re + f_im * g_im), imag + (f_re * g_im - f_im * g_re)

        return lax.fori_loop(0, share, row, carry, unroll=min(16, share))

    def make_ready(seq, slot):
        base = rows_in[other(arrival_of(seq))]

        def row(k, carry):
            start = base + rows_in[devices + k]
            for part in range(2):
                ready[block_at(slot, part, k), :] = first[pl.ds(start + part * part_rows, SUB, stride=SUB), :]
            return carry

        lax.fori_loop(0, share, row, 0, unroll=min(8, share))

    def arrival_of(seq):
        pair = seq // (2 * narrow_count)
        turn = lax.rem(seq, 2 * narrow_count) // 2
        which = lax.rem(seq, 2)
        far = jnp.where(inner, turn, swapped(turn - 1))
        mirror = jnp.where(which == 1, wide_count - 1, 0)
        away = jnp.bitwise_xor(2 * pair + lax.rem(me_w, 2), mirror) * narrow_count + far
        return jnp.where(turn == 0, (2 * pair + which) * narrow_count, away)

    def take(seq, carry):
        offset = arrival_of(seq)
        block_copy(offset).wait_recv()
        return dots(offset, carry)

    def take_ready(seq, carry):
        offset = arrival_of(seq)
        block_copy(offset).wait_recv()
        return dots_ready(seq - final, offset, carry)

    middle = devices // 2 - narrow_count
    final = devices - narrow_count
    carry = lax.fori_loop(1, middle, take, dots(0, (zero, zero)))
    squares_along_narrow()

    @pl.loop(held_back, devices - 1)
    def _(seq):
        block_copy(offset_of(seq)).start()

    @pl.loop(final, devices)
    def _(seq):
        make_ready(seq, seq - final)

    carry = lax.fori_loop(middle, final, take, carry)
    total = wait_sums(1, squares_n)
    sums[pl.ds(0, 2), :] = total
    mean_second = jnp.sum(total[1:]) / amp_total
    scale = 1.0 / jnp.sqrt(jnp.broadcast_to(mean_second, (SUB, LANE)) + 1e-06)
    send_sums(lax.fori_loop(final, devices, take_ready, carry))

    def group(i, carry):
        base = pl.multiple_of(i * (SUB * SUB), SUB * SUB)
        high = back[SUB + i]
        for r in range(SUB):
            start = high + back[r]
            for part in range(2):
                block = arrived[pl.ds(start + part * half, SUB), :]
                held[part][pl.ds(base + r, SUB, stride=SUB), :] = block * scale
        return carry

    lax.fori_loop(0, blocks_dev // SUB, group, 0, unroll=2)
    sent = pl.ds(message, (devices - 1) * message)
    pltpu.make_async_remote_copy(
        src_ref=outgoing.at[sent, :], dst_ref=arrived.at[sent, :],
        send_sem=send_sem.at[0], recv_sem=recv_sem.at[0],
        device_id=partner(1), device_id_type=MESH).wait_send()
    sums[pl.ds(2, 1), :] = wait_sums(2, totals)


def store(pieces, amp_total, held_re, held_im, sums, out_hbm, intersection_hbm, norms_hbm,
          intersection, norms, out_sem, scalar_sem):
    part_rows = held_re.shape[0]
    piece = part_rows // pieces
    copies = [pltpu.make_async_copy(held.at[pl.ds(at * piece, piece), :],
                                    out_hbm.at[pl.ds(part * part_rows + at * piece, piece), :],
                                    out_sem.at[part * pieces + at])
              for part, held in enumerate((held_re, held_im)) for at in range(pieces)]
    for copy in copies:
        copy.start()
    low = lax.broadcasted_iota(jnp.int32, (1, LANE), 1) < LANE // 2
    dots = sums[pl.ds(2, 1), :]
    parts = (sums[pl.ds(0, 1), :], sums[pl.ds(1, 1), :], jnp.where(low, dots, 0.0), jnp.where(low, 0.0, dots))
    means = [jnp.broadcast_to(jnp.sum(one) / amp_total, (SUB, LANE)) for one in parts]
    both = jnp.sqrt((means[0] + 1e-06) * (means[1] + 1e-06))
    for which in range(2):
        norms[which] = means[which][0, 0]
        intersection[which] = (means[2 + which] / both)[0, 0]
    copies.append(pltpu.make_async_copy(intersection, intersection_hbm, scalar_sem.at[0]))
    copies.append(pltpu.make_async_copy(norms, norms_hbm, scalar_sem.at[1]))
    for copy in copies[-2:]:
        copy.start()
    for copy in copies:
        copy.wait()


def local(first_state, second_state, place_first, place_second):
    blocks_dev = first_state.shape[1]
    block = first_state.shape[2]
    wide_count = lax.axis_size("wide")
    narrow_count = lax.axis_size("narrow")
    devices = wide_count * narrow_count
    share = blocks_dev // devices
    lines = 1 + bits(blocks_dev * devices) - bits(LANE)
    amp_total = float(blocks_dev * devices * block)

    def tiles(state):
        split = state.reshape(2, blocks_dev // SUB, SUB, block // LANE, LANE)
        return split.transpose(0, 1, 3, 2, 4).reshape(2 * blocks_dev * SUB, LANE)

    pieces = 4
    rows = (2 * blocks_dev * SUB, LANE)
    part = (blocks_dev * SUB, LANE)
    any_spec = pl.BlockSpec(memory_space=pl.ANY)
    hbm_spec = pl.BlockSpec(memory_space=pltpu.HBM)
    vmem_spec = pl.BlockSpec(memory_space=pltpu.VMEM)
    held = pl.pallas_call(
        functools.partial(exchange, (wide_count, narrow_count), blocks_dev, share, amp_total),
        out_shape=(pltpu.VMEM(part, jnp.float32), pltpu.VMEM(part, jnp.float32),
                   pltpu.VMEM((SUB, LANE), jnp.float32)),
        in_specs=[hbm_spec] * 4,
        out_specs=(vmem_spec,) * 3,
        scratch_shapes=[pltpu.VMEM(rows, jnp.float32)] * 3 + [
            pltpu.VMEM((narrow_count * 2 * share * SUB, LANE), jnp.float32),
            pltpu.VMEM((2, LANE), jnp.float32),
            pltpu.VMEM((wide_count, 2, LANE), jnp.float32),
            pltpu.VMEM((narrow_count, 2, LANE), jnp.float32),
            pltpu.VMEM((1, LANE), jnp.float32),
            pltpu.VMEM((devices, 1, LANE), jnp.float32),
            pltpu.SMEM((2, lines, LANE), jnp.int32),
            pltpu.SMEM((devices + share,), jnp.int32),
            pltpu.SMEM((devices + share,), jnp.int32),
            pltpu.SMEM((SUB + blocks_dev // SUB,), jnp.int32),
            pltpu.SemaphoreType.DMA((3,)),
            pltpu.SemaphoreType.DMA((2,)),
            pltpu.SemaphoreType.DMA((1,)),
            pltpu.SemaphoreType.DMA((devices,)),
            pltpu.SemaphoreType.DMA((3,)),
            pltpu.SemaphoreType.DMA((3,)),
            pltpu.SemaphoreType.REGULAR,
        ],
        compiler_params=pltpu.CompilerParams(
            collective_id=0, has_side_effects=True, vmem_limit_bytes=28 << 20),
        name="exchange",
    )(*(pltpu.with_memory_space_constraint(operand, pltpu.HBM) for operand in (
        place_first.reshape(-1, LANE), place_second.reshape(-1, LANE), tiles(first_state), tiles(second_state))))
    aligned, intersection, norms = pl.pallas_call(
        functools.partial(store, pieces, amp_total),
        out_shape=(jax.ShapeDtypeStruct(rows, jnp.float32),
                   jax.ShapeDtypeStruct((2,), jnp.float32),
                   jax.ShapeDtypeStruct((2,), jnp.float32)),
        in_specs=[vmem_spec] * 3,
        out_specs=(any_spec,) * 3,
        scratch_shapes=[
            pltpu.SMEM((2,), jnp.float32),
            pltpu.SMEM((2,), jnp.float32),
            pltpu.SemaphoreType.DMA((2 * pieces,)),
            pltpu.SemaphoreType.DMA((2,)),
        ],
        compiler_params=pltpu.CompilerParams(vmem_limit_bytes=1 << 20),
        name="store",
    )(*held)
    aligned = aligned.reshape(2, blocks_dev // SUB, block // LANE, SUB, LANE)
    aligned = aligned.transpose(0, 1, 3, 2, 4).reshape(2, blocks_dev, block)
    return (aligned, intersection, norms)


def solution(mesh):
    return jax.shard_map(
        local,
        mesh=mesh,
        in_specs=(P(None, ("wide", "narrow"), None), P(None, ("wide", "narrow"), None), P(), P()),
        out_specs=(P(None, ("wide", "narrow"), None), P(), P()),
        check_vma=False,
    )
```

```python
import functools

import jax
import jax.numpy as jnp
from jax import lax
from jax.experimental import pallas as pl
from jax.experimental.pallas import tpu as pltpu
from jax.sharding import PartitionSpec as P

MESH = pl.DeviceIdType.MESH
SUB = 8
LANE = 128


def row_weight(one_hot):
    return jnp.where(one_hot < SUB, one_hot, one_hot * SUB)


def bits(count):
    return count.bit_length() - 1


def table(ref, base, weights, start=0):
    ref[base] = jnp.int32(start)
    for level, weight in enumerate(weights):
        for low in range(1 << level):
            ref[base + (1 << level) + low] = ref[base + low] + weight


def build_out(place_f, place_s, blocks_dev, devices, share, rows_out):
    zero = jnp.int32(0)
    dev_out = [zero] * bits(devices)
    k_out = [zero] * bits(share)
    unit = jnp.int32(1)
    for level in range(bits(blocks_dev * devices)):
        f = place_f(level)
        s = place_s(level)
        f_dev = f >> bits(blocks_dev)
        both = (f_dev == 0) & ((s >> bits(blocks_dev)) == 0)
        weight = row_weight(s)
        for j in range(bits(devices)):
            dev_out[j] = dev_out[j] + jnp.where(f_dev == (1 << j), weight, 0)
        for i in range(bits(share)):
            k_out[i] = k_out[i] + jnp.where(both & (unit == (1 << i)), weight, 0)
        unit = jnp.where(both, unit * 2, unit)
    table(rows_out, 0, dev_out)
    table(rows_out, devices, k_out)


def build_in(place_f, place_s, blocks_dev, devices, me, share, rows_in, back):
    zero = jnp.int32(0)
    dev_in = [zero] * bits(devices)
    k_in = [zero] * bits(share)
    slot_back = [zero] * bits(blocks_dev)
    unit = jnp.int32(1)
    for level in range(bits(blocks_dev * devices)):
        f = place_f(level)
        s_dev = place_s(level) >> bits(blocks_dev)
        both = ((f >> bits(blocks_dev)) == 0) & (s_dev == 0)
        weight = row_weight(f)
        for j in range(bits(devices)):
            dev_in[j] = dev_in[j] + jnp.where(s_dev == (1 << j), weight, 0)
        for i in range(bits(share)):
            k_in[i] = k_in[i] + jnp.where(both & (unit == (1 << i)), weight, 0)
        toward = jnp.where((s_dev & me) == 0, s_dev, -s_dev)
        packed = jnp.where(both, unit * SUB, toward * (2 * share * SUB))
        for p in range(bits(blocks_dev)):
            slot_back[p] = slot_back[p] + jnp.where(f == (1 << p), packed, 0)
        unit = jnp.where(both, unit * 2, unit)
    table(rows_in, 0, dev_in)
    table(rows_in, devices, k_in)
    table(back, 0, slot_back[:bits(SUB)], me * (2 * share * SUB))
    table(back, SUB, slot_back[bits(SUB):])


def exchange(sizes, blocks_dev, share, amp_total, place_first, place_second, first_hbm, second_hbm,
             held_re, held_im, sums,
             first, outgoing, arrived, ready, squares, squares_w, squares_n, stats, totals, powers, rows_out, rows_in, back,
             load_sem, place_sem, send_sem, recv_sem, sum_send, sum_recv, known):
    wide_count, narrow_count = sizes
    devices = wide_count * narrow_count
    levels = bits(blocks_dev * devices)
    me_w = lax.axis_index("wide")
    me_n = lax.axis_index("narrow")
    me = me_w * narrow_count + me_n
    part_rows = blocks_dev * SUB
    half = share * SUB
    message = 2 * half
    held = (held_re, held_im)

    def partner(offset):
        return (jnp.bitwise_xor(me_w, offset // narrow_count),
                jnp.bitwise_xor(me_n, lax.rem(offset, narrow_count)))

    def other(offset):
        other_w, other_n = partner(offset)
        return other_w * narrow_count + other_n

    load_second = [pltpu.make_async_copy(second_hbm.at[pl.ds(part * part_rows, part_rows), :], held[part],
                                         load_sem.at[part]) for part in range(2)]
    load_first = pltpu.make_async_copy(first_hbm, first, load_sem.at[2])
    load_second[0].start()
    last = narrow_count - 1
    inner = (me_n != 0) & (me_n != last)
    chained = narrow_count == 4
    barrier = pltpu.get_barrier_semaphore()

    def greet(where_w, where_n):
        pl.semaphore_signal(barrier, inc=1, device_id=(where_w, where_n), device_id_type=MESH)

    if chained:
        for step in (-1, 1, 0):
            there = me_n + step

            @pl.when((there > 0) & (there < last))
            def _():
                for mate in ((0, 1) if step else (1,)):
                    greet(jnp.bitwise_xor(me_w, mate), there)

        for end in (0, last):
            @pl.loop(1, wide_count)
            def _(away):
                greet(jnp.bitwise_xor(me_w, wide_count - away), end)

            pl.when(me_n != end)(lambda: greet(me_w, end))
    else:
        @pl.loop(1, devices)
        def _(offset):
            greet(*partner(offset))

    greeted = jnp.where(inner, 5, devices - 1) if chained else devices - 1

    lines = [0] + [1 << line for line in range(levels - bits(LANE))]
    for which, place in enumerate((place_first, place_second)):
        for at, line in enumerate(lines):
            pltpu.make_async_copy(place.at[pl.ds(line, 1), :], powers.at[which, pl.ds(at, 1), :],
                                  place_sem.at[which]).start()
    load_second[1].start()
    for which, place in enumerate((place_first, place_second)):
        pltpu.make_async_copy(place.at[pl.ds(0, len(lines)), :], powers.at[which], place_sem.at[which]).wait()

    def place_of(which):
        def entry(level):
            if (1 << level) < LANE:
                return powers[which, 0, 1 << level]
            return powers[which, 1 + level - bits(LANE), 0]
        return entry

    build_out(place_of(0), place_of(1), blocks_dev, devices, share, rows_out)
    flip = jnp.where(lax.rem(me_w, 2) == 1, wide_count - 1, 0)

    def swapped(turn):
        mate = jnp.bitwise_xor(turn, 1)
        return jnp.where(mate < last, mate, turn) + 1

    odd = lax.rem(me_w, 2) == 1

    def turned(group):
        return jnp.bitwise_xor(group, 2 * jnp.bitwise_and(group, 2)) if wide_count >= 8 else group

    def offset_of(seq):
        first_far = jnp.where(inner, last, 1)
        opened = turned(jnp.int32(wide_count - 2)) * narrow_count + jnp.where(inner, last - 1, 0)
        later = seq - jnp.where(seq <= opened, 1, 0)
        at = jnp.where(odd, later, seq + jnp.where(seq < last, 0, 1))
        group = at // narrow_count
        turn = lax.rem(at, narrow_count)
        opening = last - turn
        far = jnp.where(inner, jnp.where(group == 0, opening, swapped(turn)), turn + 1)
        away = jnp.bitwise_xor(turned(group), flip) * narrow_count + far
        near = (group + jnp.where(odd, 1, 0)) * narrow_count
        return jnp.where(odd & (seq == 0), narrow_count + first_far, jnp.where(turn < last, away, near))

    def rows_at(ref, offset):
        return ref.at[pl.ds(pl.multiple_of(offset * message, message), message), :]

    def block_at(offset, part, k):
        return pl.ds(pl.multiple_of(offset * message + (part * share + k) * SUB, SUB), SUB)

    def half_copy(offset, part):
        at = pl.ds(pl.multiple_of(offset * message + part * half, half), half)
        return pltpu.make_async_remote_copy(
            src_ref=outgoing.at[at, :], dst_ref=arrived.at[at, :],
            send_sem=send_sem.at[0], recv_sem=recv_sem.at[offset],
            device_id=partner(offset), device_id_type=MESH)

    def block_copy(offset):
        return pltpu.make_async_remote_copy(
            src_ref=rows_at(outgoing, offset), dst_ref=rows_at(arrived, offset),
            send_sem=send_sem.at[0], recv_sem=recv_sem.at[offset],
            device_id=partner(offset), device_id_type=MESH)

    def pack(offset, out, parts=(0, 1)):
        base = rows_out[other(offset)]

        def row(k, carry):
            start = base + rows_out[devices + k]
            for part in parts:
                out[block_at(offset, part, k), :] = held[part][pl.ds(start, SUB, stride=SUB), :]
            return carry

        lax.fori_loop(0, share, row, 0, unroll=min(8, share))

    def pack_and_send(seq):
        pack(offset_of(seq), outgoing)
        block_copy(offset_of(seq - 1)).start()

    def sum_copy(at, src, dst, offset):
        return pltpu.make_async_remote_copy(
            src_ref=src, dst_ref=dst, send_sem=sum_send.at[at], recv_sem=sum_recv.at[at],
            device_id=partner(offset), device_id_type=MESH)

    def keep(ref, pair):
        for which in range(2):
            ref[pl.ds(which, 1), :] = jnp.sum(pair[which], axis=0, keepdims=True)

    def wait_sums(at, ref):
        every = ref.at[pl.ds(0, ref.shape[0] - 1)]
        sum_copy(at, every, every, 1).wait()
        return jnp.sum(ref[...], axis=0)

    def squares_along_wide(pair):
        keep(squares, pair)
        squares_w[me_w] = squares[...]

        @pl.loop(1, wide_count)
        def _(away):
            sum_copy(0, squares, squares_w.at[me_w], away * narrow_count).start()

    def squares_along_narrow():
        total = wait_sums(0, squares_w)
        squares[...] = total
        squares_n[me_n] = squares[...]

        @pl.loop(1, narrow_count)
        def _(plane):
            sum_copy(1, squares, squares_n.at[me_n], plane).start()

    def send_sums(pair):
        folded = [one + pltpu.roll(one, LANE // 2, 1) for one in pair]
        lane = lax.broadcasted_iota(jnp.int32, (SUB, LANE), 1)
        stats[...] = jnp.sum(jnp.where(lane < LANE // 2, folded[0], folded[1]), axis=0, keepdims=True)
        totals[me] = stats[...]

        for offset in reversed(range(1, devices)):
            sum_copy(2, stats, totals.at[me], offset).start()

    load_second[0].wait()
    pack(offset_of(0), outgoing, (0,))
    pl.semaphore_wait(barrier, greeted)
    half_copy(offset_of(0), 0).start()
    load_second[1].wait()
    load_first.start()
    pack(offset_of(0), outgoing, (1,))
    half_copy(offset_of(0), 1).start()
    if chained:
        pl.when(inner)(lambda: pl.semaphore_wait(known, 1))

        @pl.when(me_n > 1)
        def _():
            pl.semaphore_signal(known, inc=1, device_id=(me_w, me_n - 1), device_id_type=MESH)

    pack(offset_of(1), outgoing)

    early = 6
    held_back = devices - 3
    pl.loop(2, early)(pack_and_send)
    build_in(place_of(0), place_of(1), blocks_dev, devices, me, share, rows_in, back)

    load_first.wait()
    chunk = 8 * SUB

    def square(i, carry):
        at = pl.multiple_of(i * chunk, chunk)
        above = pl.multiple_of(part_rows + i * chunk, chunk)
        ones = [ref[pl.ds(start, chunk), :].reshape(chunk // SUB, SUB, LANE)
                for ref, start in ((first, at), (first, above), (held_re, at), (held_im, at))]
        squared = [jnp.sum(one * one, axis=0) for one in ones]
        return carry[0] + (squared[0] + squared[1]), carry[1] + (squared[2] + squared[3])

    zero = jnp.zeros((SUB, LANE), jnp.float32)
    squared = lax.fori_loop(0, part_rows // chunk, square, (zero, zero))
    pack_and_send(early)
    squares_along_wide(squared)
    pl.loop(early + 1, held_back + 1)(pack_and_send)

    @pl.loop(held_back + 1, devices - 1)
    def _(seq):
        pack(offset_of(seq), outgoing)

    pack(0, arrived)

    def dots(offset, carry):
        base = rows_in[other(offset)]

        def row(k, carry):
            real, imag = carry
            start = base + rows_in[devices + k]
            f_re = first[pl.ds(start, SUB, stride=SUB), :]
            f_im = first[pl.ds(start + part_rows, SUB, stride=SUB), :]
            g_re = arrived[block_at(offset, 0, k), :]
            g_im = arrived[block_at(offset, 1, k), :]
            return real + (f_re * g_re + f_im * g_im), imag + (f_re * g_im - f_im * g_re)

        return lax.fori_loop(0, share, row, carry, unroll=min(8, share))

    def dots_ready(slot, offset, carry):
        def row(k, carry):
            real, imag = carry
            f_re, f_im = (ready[block_at(slot, part, k), :] for part in range(2))
            g_re, g_im = (arrived[block_at(offset, part, k), :] for part in range(2))
            return real + (f_re * g_re + f_im * g_im), imag + (f_re * g_im - f_im * g_re)

        return lax.fori_loop(0, share, row, carry, unroll=min(16, share))

    def make_ready(seq, slot):
        base = rows_in[other(arrival_of(seq))]

        def row(k, carry):
            start = base + rows_in[devices + k]
            for part in range(2):
                ready[block_at(slot, part, k), :] = first[pl.ds(start + part * part_rows, SUB, stride=SUB), :]
            return carry

        lax.fori_loop(0, share, row, 0, unroll=min(8, share))

    def arrival_of(seq):
        pair = seq // (2 * narrow_count)
        turn = lax.rem(seq, 2 * narrow_count) // 2
        which = lax.rem(seq, 2)
        far = jnp.where(inner, turn, swapped(turn - 1))
        mirror = jnp.where(which == 1, wide_count - 1, 0)
        away = jnp.bitwise_xor(turned(2 * pair + lax.rem(me_w, 2)), mirror) * narrow_count + far
        return jnp.where(turn == 0, (2 * pair + which) * narrow_count, away)

    def take(seq, carry):
        offset = arrival_of(seq)
        block_copy(offset).wait_recv()
        return dots(offset, carry)

    def take_ready(seq, carry):
        offset = arrival_of(seq)
        block_copy(offset).wait_recv()
        return dots_ready(seq - final, offset, carry)

    middle = devices // 2 - narrow_count
    final = devices - narrow_count
    carry = lax.fori_loop(1, middle, take, dots(0, (zero, zero)))
    squares_along_narrow()

    @pl.loop(held_back, devices - 1)
    def _(seq):
        block_copy(offset_of(seq)).start()

    @pl.loop(final, devices)
    def _(seq):
        make_ready(seq, seq - final)

    carry = lax.fori_loop(middle, final, take, carry)
    total = wait_sums(1, squares_n)
    sums[pl.ds(0, 2), :] = total
    mean_second = jnp.sum(total[1:]) / amp_total
    scale = 1.0 / jnp.sqrt(jnp.broadcast_to(mean_second, (SUB, LANE)) + 1e-06)
    send_sums(lax.fori_loop(final, devices, take_ready, carry))

    def group(i, carry):
        base = pl.multiple_of(i * (SUB * SUB), SUB * SUB)
        high = back[SUB + i]
        for r in range(SUB):
            start = high + back[r]
            for part in range(2):
                block = arrived[pl.ds(start + part * half, SUB), :]
                held[part][pl.ds(base + r, SUB, stride=SUB), :] = block * scale
        return carry

    lax.fori_loop(0, blocks_dev // SUB, group, 0, unroll=2)
    sent = pl.ds(message, (devices - 1) * message)
    pltpu.make_async_remote_copy(
        src_ref=outgoing.at[sent, :], dst_ref=arrived.at[sent, :],
        send_sem=send_sem.at[0], recv_sem=recv_sem.at[0],
        device_id=partner(1), device_id_type=MESH).wait_send()
    sums[pl.ds(2, 1), :] = wait_sums(2, totals)


def store(pieces, amp_total, held_re, held_im, sums, out_hbm, intersection_hbm, norms_hbm,
          intersection, norms, out_sem, scalar_sem):
    part_rows = held_re.shape[0]
    piece = part_rows // pieces
    copies = [pltpu.make_async_copy(held.at[pl.ds(at * piece, piece), :],
                                    out_hbm.at[pl.ds(part * part_rows + at * piece, piece), :],
                                    out_sem.at[part * pieces + at])
              for part, held in enumerate((held_re, held_im)) for at in range(pieces)]
    for copy in copies:
        copy.start()
    low = lax.broadcasted_iota(jnp.int32, (1, LANE), 1) < LANE // 2
    dots = sums[pl.ds(2, 1), :]
    parts = (sums[pl.ds(0, 1), :], sums[pl.ds(1, 1), :], jnp.where(low, dots, 0.0), jnp.where(low, 0.0, dots))
    means = [jnp.broadcast_to(jnp.sum(one) / amp_total, (SUB, LANE)) for one in parts]
    both = jnp.sqrt((means[0] + 1e-06) * (means[1] + 1e-06))
    for which in range(2):
        norms[which] = means[which][0, 0]
        intersection[which] = (means[2 + which] / both)[0, 0]
    copies.append(pltpu.make_async_copy(intersection, intersection_hbm, scalar_sem.at[0]))
    copies.append(pltpu.make_async_copy(norms, norms_hbm, scalar_sem.at[1]))
    for copy in copies[-2:]:
        copy.start()
    for copy in copies:
        copy.wait()


def local(first_state, second_state, place_first, place_second):
    blocks_dev = first_state.shape[1]
    block = first_state.shape[2]
    wide_count = lax.axis_size("wide")
    narrow_count = lax.axis_size("narrow")
    devices = wide_count * narrow_count
    share = blocks_dev // devices
    lines = 1 + bits(blocks_dev * devices) - bits(LANE)
    amp_total = float(blocks_dev * devices * block)

    def tiles(state):
        split = state.reshape(2, blocks_dev // SUB, SUB, block // LANE, LANE)
        return split.transpose(0, 1, 3, 2, 4).reshape(2 * blocks_dev * SUB, LANE)

    pieces = 4
    rows = (2 * blocks_dev * SUB, LANE)
    part = (blocks_dev * SUB, LANE)
    any_spec = pl.BlockSpec(memory_space=pl.ANY)
    hbm_spec = pl.BlockSpec(memory_space=pltpu.HBM)
    vmem_spec = pl.BlockSpec(memory_space=pltpu.VMEM)
    held = pl.pallas_call(
        functools.partial(exchange, (wide_count, narrow_count), blocks_dev, share, amp_total),
        out_shape=(pltpu.VMEM(part, jnp.float32), pltpu.VMEM(part, jnp.float32),
                   pltpu.VMEM((SUB, LANE), jnp.float32)),
        in_specs=[hbm_spec] * 4,
        out_specs=(vmem_spec,) * 3,
        scratch_shapes=[pltpu.VMEM(rows, jnp.float32)] * 3 + [
            pltpu.VMEM((narrow_count * 2 * share * SUB, LANE), jnp.float32),
            pltpu.VMEM((2, LANE), jnp.float32),
            pltpu.VMEM((wide_count, 2, LANE), jnp.float32),
            pltpu.VMEM((narrow_count, 2, LANE), jnp.float32),
            pltpu.VMEM((1, LANE), jnp.float32),
            pltpu.VMEM((devices, 1, LANE), jnp.float32),
            pltpu.SMEM((2, lines, LANE), jnp.int32),
            pltpu.SMEM((devices + share,), jnp.int32),
            pltpu.SMEM((devices + share,), jnp.int32),
            pltpu.SMEM((SUB + blocks_dev // SUB,), jnp.int32),
            pltpu.SemaphoreType.DMA((3,)),
            pltpu.SemaphoreType.DMA((2,)),
            pltpu.SemaphoreType.DMA((1,)),
            pltpu.SemaphoreType.DMA((devices,)),
            pltpu.SemaphoreType.DMA((3,)),
            pltpu.SemaphoreType.DMA((3,)),
            pltpu.SemaphoreType.REGULAR,
        ],
        compiler_params=pltpu.CompilerParams(
            collective_id=0, has_side_effects=True, vmem_limit_bytes=28 << 20),
        name="exchange",
    )(*(pltpu.with_memory_space_constraint(operand, pltpu.HBM) for operand in (
        place_first.reshape(-1, LANE), place_second.reshape(-1, LANE), tiles(first_state), tiles(second_state))))
    aligned, intersection, norms = pl.pallas_call(
        functools.partial(store, pieces, amp_total),
        out_shape=(jax.ShapeDtypeStruct(rows, jnp.float32),
                   jax.ShapeDtypeStruct((2,), jnp.float32),
                   jax.ShapeDtypeStruct((2,), jnp.float32)),
        in_specs=[vmem_spec] * 3,
        out_specs=(any_spec,) * 3,
        scratch_shapes=[
            pltpu.SMEM((2,), jnp.float32),
            pltpu.SMEM((2,), jnp.float32),
            pltpu.SemaphoreType.DMA((2 * pieces,)),
            pltpu.SemaphoreType.DMA((2,)),
        ],
        compiler_params=pltpu.CompilerParams(vmem_limit_bytes=1 << 20),
        name="store",
    )(*held)
    aligned = aligned.reshape(2, blocks_dev // SUB, block // LANE, SUB, LANE)
    aligned = aligned.transpose(0, 1, 3, 2, 4).reshape(2, blocks_dev, block)
    return (aligned, intersection, norms)


def solution(mesh):
    return jax.shard_map(
        local,
        mesh=mesh,
        in_specs=(P(None, ("wide", "narrow"), None), P(None, ("wide", "narrow"), None), P(), P()),
        out_specs=(P(None, ("wide", "narrow"), None), P(), P()),
        check_vma=False,
    )
```
